32 devices in a mesh: rep: 2 (over x), emb: 4 (over z), model: 4 (over y, core).
Axes of the slice: x: 2, y: 2, z: 4, core: 2. Of those that a mesh axis runs over, the one named last changes fastest.
Arguments:
- x: bfloat16 [1024, 2048], P('rep'), parts along dimension 0
- Wq: bfloat16 [2048, 2048], P('emb', 'model')
- Wk: bfloat16 [2048, 256], replicated
- Wv: bfloat16 [2048, 256], replicated
- Wo: bfloat16 [2048, 2048], P('model', 'emb')
- Kc: bfloat16 [1024, 1024, 256], P('rep'), parts along dimension 0
- Vc: bfloat16 [1024, 1024, 256], P('rep'), parts along dimension 0
- lengths: int32 [1024], P('rep'), parts along dimension 0
Outputs:
- output 1: bfloat16 [1024, 2048], P('rep'), parts along dimension 0
- output 2: bfloat16 [1024, 256], P('rep'), parts along dimension 0
- output 3: bfloat16 [1024, 256], P('rep'), parts along dimension 0
There are 2 independent parts. The reference program is written for one: setup_inputs(seed, part) draws one part's arguments, and reference() takes and returns one part's arrays. A program takes and returns all parts, laid end to end along the dimension named above; an argument that names none is the same for every part.
All inputs are finite; a program needn't handle non-finite values.
Results may differ from the reference program's by a relative error of at most 0.0109362.
Values are sent between devices in bfloat16 or wider.
A program may use at most 2.25 GiB of HBM per device.

```python
import jax
import jax.numpy as jnp
from jax import lax

B = 512
T = 1024
D = 2048
H = 8
DH = 256


def setup_inputs(seed: int = 0, part: int = 0) -> dict:
    kshared, kpart = jax.random.split(jax.random.key(seed))
    kpart = jax.random.fold_in(kpart, part)
    kq, kk, kv, ko = jax.random.split(kshared, 4)
    kx, kkc, kvc, kl = jax.random.split(kpart, 4)
    x = jax.random.normal(kx, (B, D), jnp.float32)
    Wq = jax.random.normal(kq, (D, H * DH), jnp.float32) * (2.5 * D ** -0.5)
    Wk = jax.random.normal(kk, (D, DH), jnp.float32) * D ** -0.5
    Wv = jax.random.normal(kv, (D, DH), jnp.float32) * D ** -0.5
    Wo = jax.random.normal(ko, (H * DH, D), jnp.float32) * (3.0 * (H * DH) ** -0.5)
    Kc = jax.random.normal(kkc, (B, T, DH), jnp.float32)
    Vc = jax.random.normal(kvc, (B, T, DH), jnp.float32)
    kl1, kl2, kl3 = jax.random.split(jax.random.fold_in(kl, 7), 3)
    full = T - 1 - jax.random.randint(kl1, (B,), 0, T // 8)
    tiny = jax.random.randint(kl2, (B,), 1, 9)
    lengths = jnp.where(jax.random.bernoulli(kl3, 0.5, (B,)), full, tiny).astype(jnp.int32)
    bf = jnp.bfloat16
    return {'x': x.astype(bf), 'Wq': Wq.astype(bf), 'Wk': Wk.astype(bf), 'Wv': Wv.astype(bf),
            'Wo': Wo.astype(bf), 'Kc': Kc.astype(bf), 'Vc': Vc.astype(bf), 'lengths': lengths}


def reference(x, Wq, Wk, Wv, Wo, Kc, Vc, lengths):
    scale = DH ** -0.5
    q = jnp.dot(x, Wq, preferred_element_type=jnp.float32).astype(jnp.bfloat16).reshape(B, H, DH)
    k_new = jnp.dot(x, Wk, preferred_element_type=jnp.float32).astype(jnp.bfloat16)
    v_new = jnp.dot(x, Wv, preferred_element_type=jnp.float32).astype(jnp.bfloat16)
    pos = jnp.arange(T)

    def one(a):
        qb, Kb, Vb, kn, vn, n = a
        s = jnp.dot(qb, Kb.T, preferred_element_type=jnp.float32) * scale
        s = jnp.where(pos[None, :] < n, s, -jnp.inf)
        sn = jnp.dot(qb, kn, preferred_element_type=jnp.float32) * scale
        m = jnp.maximum(jnp.max(s, axis=1), sn)
        p = jnp.exp(s - m[:, None])
        pn = jnp.exp(sn - m)
        l = jnp.sum(p, axis=1) + pn
        acc = jnp.dot(p.astype(jnp.bfloat16), Vb, preferred_element_type=jnp.float32)
        acc = acc + pn.astype(jnp.bfloat16).astype(jnp.float32)[:, None] * vn.astype(jnp.float32)[None, :]
        return (acc / l[:, None]).astype(jnp.bfloat16)

    o = lax.map(one, (q, Kc, Vc, k_new, v_new, lengths))
    y = x.astype(jnp.float32) + jnp.dot(o.reshape(B, H * DH), Wo, preferred_element_type=jnp.float32)
    return y.astype(jnp.bfloat16), k_new, v_new
```

```python
import functools

import jax
import jax.numpy as jnp
from jax import lax
from jax.experimental import pallas as pl
from jax.experimental.pallas import tpu as pltpu
from jax.sharding import PartitionSpec as P

BF = jnp.bfloat16
F32 = jnp.float32
NB = 2
UNROLL = 4
CHUNK = 8


def _kernel(x_h, wq_h, wk_h, wv_h, wo_h, kc_h, vc_h, lens,
            y_h, kn_h, vn_h,
            x_v, wq_v, wall, wk_v, wv_v, wo_v, k_v, v_v, kn_v, vn_v, knf, vnf,
            qacc, q_my, q_in, qf, of, o_in, y_v,
            lsem, ksem, vsem, osem,
            a_s, a_r, x_s, x_r, c_s, c_r, w_s, w_r, o_s, o_r,
            yz_s, yz_r, yy_s, yy_r, yd_s, yd_r):
    r = lax.axis_index('rep')
    z = lax.axis_index('emb')
    m = lax.axis_index('model')
    yy = m // 2
    c = m % 2
    my = yy * 2 + 1 - c
    mx = (1 - yy) * 2 + c
    me = z * 4 + m
    bl = k_v.shape[0]
    nb = bl // NB
    t = k_v.shape[1]
    dh = k_v.shape[2]
    nh = 8
    half = dh // 2
    de = wq_v.shape[0]
    hr = de // 2
    start = pl.multiple_of(me * bl, bl)
    scale = dh ** -0.5

    def rcopy(src, dst, ss, rs, rr, zz, mm):
        return pltpu.make_async_remote_copy(
            src_ref=src, dst_ref=dst, send_sem=ss, recv_sem=rs,
            device_id=(rr, zz, mm), device_id_type=pl.DeviceIdType.MESH)

    ld_wq = pltpu.make_async_copy(wq_h, wq_v, lsem.at[0])
    ld_x = pltpu.make_async_copy(x_h, x_v, lsem.at[1])
    ld_wk = pltpu.make_async_copy(wk_h, wk_v, lsem.at[2])
    ld_wv = pltpu.make_async_copy(wv_h, wv_v, lsem.at[3])
    ld_wo = pltpu.make_async_copy(wo_h, wo_v.at[m], lsem.at[4])
    ld_wq.start()
    ld_x.start()
    ld_wk.start()
    ld_wv.start()
    ld_wo.start()
    kcp, vcp = [], []
    for i in range(bl // CHUNK):
        src = pl.ds(start + i * CHUNK, CHUNK)
        dst = pl.ds(i * CHUNK, CHUNK)
        kcp.append(pltpu.make_async_copy(kc_h.at[src], k_v.at[dst], ksem.at[i]))
        vcp.append(pltpu.make_async_copy(vc_h.at[src], v_v.at[dst], vsem.at[i]))
    for i in range(bl // CHUNK):
        kcp[i].start()
        vcp[i].start()

    barrier = pltpu.get_barrier_semaphore()
    for k in range(1, 16):
        p = lax.rem(me + k, 16)
        pl.semaphore_signal(barrier, inc=1, device_id=(r, p // 4, p % 4),
                            device_id_type=pl.DeviceIdType.MESH)
    pl.semaphore_signal(barrier, inc=1, device_id=(1 - r, z, m),
                        device_id_type=pl.DeviceIdType.MESH)
    pl.semaphore_wait(barrier, 16)

    ld_wq.wait()
    ld_wq_rows = pl.ds(pl.multiple_of(r * hr, hr), hr)

    def a_half(tt, cd, i):
        zd = 2 * c + tt
        cols = pl.ds(tt * dh + cd * half, half)
        return rcopy(wq_v.at[ld_wq_rows, cols], wall.at[z, ld_wq_rows, :], a_s.at[i], a_r.at[z],
                     r, zd, yy * 2 + cd)

    def a_full(tt, cd, i):
        cols = pl.ds(tt * dh + cd * half, half)
        return rcopy(wq_v.at[:, cols], wall.at[z], a_s.at[i], a_r.at[z],
                     r, z, yy * 2 + cd)

    def a_self(tt, cd, i):
        cols = pl.ds(tt * dh + cd * half, half)
        return pltpu.make_async_copy(wq_v.at[:, cols], wall.at[z], a_s.at[i])

    def a_each(fn):
        for tt in range(2):
            for cd in range(2):
                i = tt * 2 + cd
                zd = 2 * c + tt

                @pl.when(zd != z)
                def _():
                    fn(a_half(tt, cd, i), False)

                @pl.when((zd == z) & (c != cd))
                def _():
                    fn(a_full(tt, cd, i), False)

                @pl.when((zd == z) & (c == cd))
                def _():
                    fn(a_self(tt, cd, i), True)

    a_each(lambda d, own: d.start())

    ld_wo.wait()
    wo_y = rcopy(wo_v.at[m], wo_v.at[m], w_s.at[0], w_r.at[0], r, z, mx)
    wo_d = rcopy(wo_v.at[m], wo_v.at[m], w_s.at[1], w_r.at[1], r, z, my)
    wo_y.start()
    wo_d.start()

    ld_x.wait()
    ld_wk.wait()
    kn_v[...] = jnp.dot(x_v[...], wk_v[...], preferred_element_type=F32).astype(BF)
    ld_wv.wait()
    vn_v[...] = jnp.dot(x_v[...], wv_v[...], preferred_element_type=F32).astype(BF)
    st_kn = pltpu.make_async_copy(kn_v, kn_h, osem.at[0])
    st_vn = pltpu.make_async_copy(vn_v, vn_h, osem.at[1])
    st_kn.start()
    st_vn.start()
    knf[...] = kn_v[pl.ds(start, bl), :].astype(F32)
    vnf[...] = vn_v[pl.ds(start, bl), :].astype(F32)

    ms = yy * 2 + z // 2

    def a_rec(zs):
        return rcopy(wall.at[zs, ld_wq_rows, :], wall.at[zs, ld_wq_rows, :], a_s.at[0], a_r.at[zs],
                     r, zs, ms)

    def x_fwd(zs):
        return rcopy(wall.at[zs, ld_wq_rows, :], wall.at[zs, ld_wq_rows, :], x_s.at[zs], x_r.at[zs],
                     1 - r, z, m)

    other = pl.ds(pl.multiple_of((1 - r) * hr, hr), hr)

    def x_rec(zs):
        return rcopy(wall.at[zs, other, :], wall.at[zs, other, :], x_s.at[zs], x_r.at[zs],
                     1 - r, z, m)

    def qdot(zs):
        cols = pl.ds(pl.multiple_of(zs * de, de), de)
        return jnp.dot(x_v[:, cols], wall[zs], preferred_element_type=F32)

    @pl.when(ms == m)
    def _():
        for tt in range(2):
            for cd in range(2):
                @pl.when((2 * c + tt == z) & (cd == c))
                def _():
                    a_self(tt, cd, tt * 2 + cd).wait()

    @pl.when(ms != m)
    def _():
        rcopy(wall.at[z], wall.at[z], a_s.at[0], a_r.at[z], r, z, my).wait_recv()

    qacc[...] = qdot(z)
    for k in range(1, 4):
        zs = lax.rem(z + k, 4)
        a_rec(zs).wait_recv()
        x_fwd(zs).start()
    for k in range(1, 4):
        zs = lax.rem(z + k, 4)
        x_rec(zs).wait_recv()
        qacc[...] += qdot(zs)
    q_my[...] = qacc[...].astype(BF).reshape(q_my.shape)

    slot = (4 * yy + z) * 2 + c
    for k in range(1, 16):
        p = lax.rem(me + k, 16)
        rcopy(q_my.at[p], q_in.at[slot], c_s.at[k - 1], c_r.at[slot], r, p // 4, p % 4).start()
    q_in[slot] = q_my[me]

    rcopy(wo_v.at[mx], wo_v.at[mx], w_s.at[0], w_r.at[0], r, z, mx).wait_recv()
    wo_f = rcopy(wo_v.at[mx], wo_v.at[mx], w_s.at[2], w_r.at[2], r, z, my)
    wo_f.start()

    for k in range(1, 16):
        s_ = lax.rem(slot + k, 16)
        rcopy(q_in.at[s_], q_in.at[s_], c_s.at[k - 1], c_r.at[s_], r, z, m).wait_recv()
    qf[...] = q_in[...].astype(F32).reshape(qf.shape)

    lane = lax.broadcasted_iota(jnp.int32, (nh, t), 1)

    def attend(base, bb):
        b = base + bb
        q = jnp.concatenate([qf[pl.ds(b, nh, stride=2 * bl), :],
                             qf[pl.ds(b + bl, nh, stride=2 * bl), :]], axis=1)
        s = lax.dot_general(q.astype(BF), k_v[b], (((1,), (1,)), ((), ())),
                            preferred_element_type=F32) * scale
        s = jnp.where(lane < lens[start + b], s, -jnp.inf)
        sn = jnp.sum(q * knf[pl.ds(b, 1), :], axis=1, keepdims=True) * scale
        mx_ = jnp.maximum(jnp.max(s, axis=1, keepdims=True), sn)
        p = jnp.exp(s - mx_)
        pn = jnp.exp(sn - mx_)
        l = jnp.sum(p, axis=1, keepdims=True) + pn
        acc = jnp.dot(p.astype(BF), v_v[b], preferred_element_type=F32)
        acc = acc + pn.astype(BF).astype(F32) * vnf[pl.ds(b, 1), :]
        return acc / l

    oz = pl.ds(pl.multiple_of(z * nb, nb), nb)

    def o_send(n, k):
        zd = lax.rem(z + k, 4)
        return rcopy(o_in.at[n, :, oz, :], o_in.at[n, :, oz, :], o_s.at[n, k - 1], o_r.at[n, z],
                     r, zd, m)

    def o_rec(n, zs):
        rows = pl.ds(pl.multiple_of(zs * nb, nb), nb)
        return rcopy(o_in.at[n, :, rows, :], o_in.at[n, :, rows, :], o_s.at[n, 0], o_r.at[n, zs],
                     r, zs, m)

    for n in range(NB):
        for i in range(nb // CHUNK):
            kcp[n * (nb // CHUNK) + i].wait()
            vcp[n * (nb // CHUNK) + i].wait()

        def group(g, carry):
            for u in range(UNROLL):
                bb = g * UNROLL + u
                o = attend(n * nb, bb)
                of[0, pl.ds(bb, nh, stride=nb), :] = o[:, :half]
                of[1, pl.ds(bb, nh, stride=nb), :] = o[:, half:]
            return carry

        lax.fori_loop(0, nb // UNROLL, group, 0)
        for h in range(nh):
            rows = slice(h * nb, (h + 1) * nb)
            o_in[n, h, oz, :] = jnp.concatenate([of[0, rows, :], of[1, rows, :]], axis=1).astype(BF)
        for k in range(1, 4):
            o_send(n, k).start()

    rcopy(wo_v.at[my], wo_v.at[my], w_s.at[1], w_r.at[1], r, z, my).wait_recv()
    md = (1 - yy) * 2 + 1 - c
    rcopy(wo_v.at[md], wo_v.at[md], w_s.at[2], w_r.at[2], r, z, my).wait_recv()

    def blk(n, zs, ms_):
        return y_v.at[:, ms_, pl.ds(n * nb, nb), pl.ds(pl.multiple_of(zs * de, de), de)]

    def yz_send(n, k):
        zd = lax.rem(z + k, 4)
        return rcopy(blk(n, z, m), blk(n, z, m), yz_s.at[n, k - 1], yz_r.at[n, z], r, zd, m)

    def yz_rec(n, zs):
        return rcopy(blk(n, zs, m), blk(n, zs, m), yz_s.at[n, 0], yz_r.at[n, zs], r, zs, m)

    def yy_send(n, zs):
        return rcopy(blk(n, zs, m), blk(n, zs, m), yy_s.at[n, zs], yy_r.at[n, zs], r, z, mx)

    def yy_rec(n, zs):
        return rcopy(blk(n, zs, mx), blk(n, zs, mx), yy_s.at[n, zs], yy_r.at[n, zs], r, z, mx)

    def yd_send(n, zs, hop):
        ms_ = mx if hop else m
        return rcopy(blk(n, zs, ms_), blk(n, zs, ms_), yd_s.at[n, hop, zs], yd_r.at[n, hop, zs],
                     r, z, my)

    def yd_rec(n, zs, hop):
        ms_ = md if hop else my
        return rcopy(blk(n, zs, ms_), blk(n, zs, ms_), yd_s.at[n, hop, zs], yd_r.at[n, hop, zs],
                     r, z, my)

    for n in range(NB):
        for k in range(1, 4):
            o_rec(n, lax.rem(z + k, 4)).wait_recv()
        acc = jnp.zeros((4 * nb, de), F32)
        for h in range(nh):
            acc = acc + jnp.dot(o_in[n, h], wo_v[h // 2, (h % 2) * dh:(h % 2 + 1) * dh, :],
                                preferred_element_type=F32)
        zc = pl.ds(pl.multiple_of(z * de, de), de)
        for zs in range(4):
            rows = pl.ds(pl.multiple_of(zs * 4 * bl + m * bl + n * nb, nb), nb)
            yb = x_v[rows, zc].astype(F32) + acc[zs * nb:(zs + 1) * nb]
            y_v[zs, m, n * nb:(n + 1) * nb, zc] = yb.astype(BF)
        for k in range(1, 4):
            yz_send(n, k).start()
        yy_send(n, z).start()
        yd_send(n, z, 0).start()

    for n in range(NB):
        for k in range(1, 4):
            zs = lax.rem(z + k, 4)
            yz_rec(n, zs).wait_recv()
            yy_send(n, zs).start()
            yd_send(n, zs, 0).start()
    for n in range(NB):
        for k in range(4):
            zs = lax.rem(z + k, 4)
            yy_rec(n, zs).wait_recv()
            yd_send(n, zs, 1).start()
    for n in range(NB):
        for hop in range(2):
            for k in range(4):
                yd_rec(n, lax.rem(z + k, 4), hop).wait_recv()

    st_y = pltpu.make_async_copy(y_v, y_h, osem.at[2])
    st_y.start()

    a_each(lambda d, own: None if own else d.wait_send())
    for k in range(1, 4):
        x_fwd(lax.rem(z + k, 4)).wait_send()
    for k in range(1, 16):
        p = lax.rem(me + k, 16)
        rcopy(q_my.at[p], q_in.at[slot], c_s.at[k - 1], c_r.at[slot], r, p // 4, p % 4).wait_send()
    wo_y.wait_send()
    wo_d.wait_send()
    wo_f.wait_send()
    for n in range(NB):
        for k in range(1, 4):
            o_send(n, k).wait_send()
            yz_send(n, k).wait_send()
        for zs in range(4):
            yy_send(n, zs).wait_send()
            yd_send(n, zs, 0).wait_send()
            yd_send(n, zs, 1).wait_send()
    st_kn.wait()
    st_vn.wait()
    st_y.wait()


def solution(mesh):
    ne = mesh.shape['emb']
    nm = mesh.shape['model']

    def local(x, Wq, Wk, Wv, Wo, Kc, Vc, lengths):
        b, d = x.shape
        t, dh = Kc.shape[1:]
        de = Wq.shape[0]
        bl = b // (ne * nm)
        nb = bl // NB
        nh = 8
        hbm = pl.BlockSpec(memory_space=pl.ANY)
        dma = pltpu.SemaphoreType.DMA
        y, kn, vn = pl.pallas_call(
            _kernel,
            out_shape=(jax.ShapeDtypeStruct((ne, nm, bl, d), BF),
                       jax.ShapeDtypeStruct((b, dh), BF),
                       jax.ShapeDtypeStruct((b, dh), BF)),
            in_specs=[hbm] * 7 + [pl.BlockSpec(memory_space=pltpu.SMEM)],
            out_specs=(hbm, hbm, hbm),
            scratch_shapes=[
                pltpu.VMEM((b, d), BF), pltpu.VMEM(Wq.shape, BF), pltpu.VMEM((ne, de, dh // 2), BF),
                pltpu.VMEM(Wk.shape, BF), pltpu.VMEM(Wv.shape, BF), pltpu.VMEM((nm,) + Wo.shape, BF),
                pltpu.VMEM((bl, t, dh), BF), pltpu.VMEM((bl, t, dh), BF),
                pltpu.VMEM((b, dh), BF), pltpu.VMEM((b, dh), BF),
                pltpu.VMEM((bl, dh), F32), pltpu.VMEM((bl, dh), F32),
                pltpu.VMEM((b, dh // 2), F32),
                pltpu.VMEM((16, bl, dh // 2), BF), pltpu.VMEM((16, bl, dh // 2), BF),
                pltpu.VMEM((16 * bl, dh // 2), F32),
                pltpu.VMEM((2, nh * nb, dh // 2), F32),
                pltpu.VMEM((NB, nh, ne * nb, dh), BF),
                pltpu.VMEM((ne, nm, bl, d), BF),
                dma((5,)), dma((bl // CHUNK,)), dma((bl // CHUNK,)), dma((3,)),
                dma((4,)), dma((4,)), dma((4,)), dma((4,)),
                dma((15,)), dma((16,)), dma((3,)), dma((3,)),
                dma((NB, 3)), dma((NB, 4)),
                dma((NB, 3)), dma((NB, 4)), dma((NB, 4)), dma((NB, 4)),
                dma((NB, 2, 4)), dma((NB, 2, 4)),
            ],
            compiler_params=pltpu.CompilerParams(
                collective_id=0, has_side_effects=True, vmem_limit_bytes=60 * 1024 * 1024),
        )(x, Wq, Wk, Wv, Wo, Kc, Vc, lengths)
        return y.reshape(b, d), kn, vn

    in_specs = (P('rep', None), P('emb', 'model'), P(), P(), P('model', 'emb'),
                P('rep', None, None), P('rep', None, None), P('rep'))
    out_specs = (P('rep', None), P('rep', None), P('rep', None))
    return jax.shard_map(local, mesh=mesh, in_specs=in_specs, out_specs=out_specs, check_vma=False)
```

```python
import functools

import jax
import jax.numpy as jnp
from jax import lax
from jax.experimental import pallas as pl
from jax.experimental.pallas import tpu as pltpu
from jax.sharding import PartitionSpec as P

BF = jnp.bfloat16
F32 = jnp.float32
NB = 4
J0 = 160
LAG = 2
VMEM_LIMIT = 54 * 1024 * 1024
CHUNK = 8


def _kernel(x_h, wq_h, wk_h, wv_h, wo_h, kc_h, vc_h, lens,
            y_v, kn_v, vn_v,
            x_v, wq_v, wall, wk_v, wv_v, wst, wo_v, k_v, v_v, knf, vnf,
            qacc, q_my, q_in, qf, of, o_in,
            lsem, ksem, vsem,
            a_s, a_r, x_s, x_r, c_s, c_r, w1_s, w1_r, w2_s, w3_s, wn_s, wt_s, wn_r, wt_r,
            o_s, o_r, yz_s, yz_r, yy_s, yy_r, yd_s, yd_r):
    r = lax.axis_index('rep')
    z = lax.axis_index('emb')
    m = lax.axis_index('model')
    yy = m // 2
    c = m % 2
    my = yy * 2 + 1 - c
    mx = (1 - yy) * 2 + c
    near = z + 1 - 2 * (z % 2)
    z2 = lax.rem(z + 2, 4)
    me = z * 4 + m
    bl = k_v.shape[0]
    nb = bl // NB
    t = k_v.shape[1]
    dh = k_v.shape[2]
    nh = 8
    half = dh // 2
    de = wq_v.shape[0]
    hr = de // 2
    start = pl.multiple_of(me * bl, bl)
    scale = dh ** -0.5

    def rcopy(src, dst, ss, rs, rr, zz, mm):
        return pltpu.make_async_remote_copy(
            src_ref=src, dst_ref=dst, send_sem=ss, recv_sem=rs,
            device_id=(rr, zz, mm), device_id_type=pl.DeviceIdType.MESH)

    ld_wq = pltpu.make_async_copy(wq_h, wq_v, lsem.at[0])
    ld_x = pltpu.make_async_copy(x_h, x_v, lsem.at[1])
    ld_wk = pltpu.make_async_copy(wk_h, wk_v, lsem.at[2])
    ld_wv = pltpu.make_async_copy(wv_h, wv_v, lsem.at[3])
    ld_wo = pltpu.make_async_copy(wo_h, wst, lsem.at[4])
    ld_wq.start()
    ld_x.start()
    ld_wk.start()
    ld_wv.start()
    ld_wo.start()
    kcp, vcp = [], []
    for i in range(bl // CHUNK):
        src = pl.ds(start + i * CHUNK, CHUNK)
        dst = pl.ds(i * CHUNK, CHUNK)
        kcp.append(pltpu.make_async_copy(kc_h.at[src], k_v.at[dst], ksem.at[i]))
        vcp.append(pltpu.make_async_copy(vc_h.at[src], v_v.at[dst], vsem.at[i]))

    barrier = pltpu.get_barrier_semaphore()
    for k in range(1, 16):
        p = lax.rem(me + k, 16)
        pl.semaphore_signal(barrier, inc=1, device_id=(r, p // 4, p % 4),
                            device_id_type=pl.DeviceIdType.MESH)
    pl.semaphore_signal(barrier, inc=1, device_id=(1 - r, z, m),
                        device_id_type=pl.DeviceIdType.MESH)
    pl.semaphore_wait(barrier, 16)

    ld_wq.wait()
    ld_wq_rows = pl.ds(pl.multiple_of(r * hr, hr), hr)

    def a_half(tt, cd, i):
        zd = 2 * c + tt
        cols = pl.ds(tt * dh + cd * half, half)
        return rcopy(wq_v.at[ld_wq_rows, cols], wall.at[z, ld_wq_rows, :], a_s.at[i], a_r.at[z],
                     r, zd, yy * 2 + cd)

    def a_full(tt, cd, i):
        cols = pl.ds(tt * dh + cd * half, half)
        return rcopy(wq_v.at[:, cols], wall.at[z], a_s.at[i], a_r.at[z],
                     r, z, yy * 2 + cd)

    def a_self(tt, cd, i):
        cols = pl.ds(tt * dh + cd * half, half)
        return pltpu.make_async_copy(wq_v.at[:, cols], wall.at[z], a_s.at[i])

    def a_each(fn):
        for first in range(2):
            @pl.when(z % 2 == first)
            def _():
                for tt in (first, 1 - first):
                    for cd in range(2):
                        i = tt * 2 + cd
                        zd = 2 * c + tt

                        @pl.when(zd != z)
                        def _():
                            fn(a_half(tt, cd, i), False)

                        @pl.when((zd == z) & (c != cd))
                        def _():
                            fn(a_full(tt, cd, i), False)

                        @pl.when((zd == z) & (c == cd))
                        def _():
                            fn(a_self(tt, cd, i), True)

    a_each(lambda d, own: d.start())

    far = c != z // 2
    ld_wo.wait()
    w_own = pltpu.make_async_copy(wst, wo_v.at[m], lsem.at[5])
    w_d2d = rcopy(wst, wo_v.at[m], w1_s.at[0], w1_r.at[0], r, z, my)

    def w_y(i):
        rows = pl.ds(i * hr, hr)
        return rcopy(wst.at[rows, :], wo_v.at[m, rows, :], w2_s.at[i], wn_r.at[m, i],
                     r, z, (1 - yy) * 2 + z // 2)

    def w_rows(g, j):
        return pl.ds(pl.multiple_of(g * hr + j * J0, 16), hr - J0 if j else J0)

    def w_z(j):
        return rcopy(wst.at[w_rows(r, j), :], wo_v.at[m, w_rows(r, j), :], w3_s.at[j], wn_r.at[m, j],
                     r, z2, yy * 2 + z // 2)

    def w_half(mm, j):
        return wo_v.at[mm, w_rows(r, j), :]

    def w_next(k, j):
        mm = 2 * yy + k
        return rcopy(w_half(mm, j), w_half(mm, j), wn_s.at[k, j], wn_r.at[mm, j], r, z, mx)

    def w_twin(mm, j):
        return rcopy(w_half(mm, j), w_half(mm, j), wt_s.at[mm, j], wt_r.at[mm, j], 1 - r, z, m)

    def w_arrived(mm, j):
        return rcopy(w_half(mm, j), w_half(mm, j), wt_s.at[mm, j], wn_r.at[mm, j], r, z, mx)

    def w_pass_z(j):
        @pl.when(far)
        def _():
            for k in range(2):
                w_arrived(2 * yy + k, j).wait_recv()
                w_next(k, j).start()
                w_twin(2 * yy + k, j).start()

    def w_pass_y(j):
        @pl.when(far)
        def _():
            for k in range(2):
                w_arrived(2 * (1 - yy) + k, j).wait_recv()
                w_twin(2 * (1 - yy) + k, j).start()

    def w_wait():
        @pl.when(far)
        def _():
            for mm in range(4):
                for j in range(2):
                    part = wo_v.at[mm, w_rows(1 - r, j), :]
                    rcopy(part, part, wt_s.at[mm, j], wt_r.at[mm, j], 1 - r, z, m).wait_recv()

        @pl.when(~far)
        def _():
            w_own.wait()
            rcopy(wst, wo_v.at[my], w1_s.at[0], w1_r.at[0], r, z, my).wait_recv()
            for k in range(2):
                for i in range(2):
                    part = wo_v.at[2 * (1 - yy) + k, pl.ds(i * hr, hr), :]
                    rcopy(part, part, w2_s.at[i], wn_r.at[2 * (1 - yy) + k, i], r, z, mx).wait_recv()

    @pl.when(far)
    def _():
        w_d2d.start()

    @pl.when(~far)
    def _():
        w_own.start()

    w_z(0).start()
    w_y(0).start()

    ld_x.wait()
    ld_wk.wait()
    ld_wv.wait()
    for i in range(bl // CHUNK):
        kcp[i].start()
        vcp[i].start()
    kn_v[...] = jnp.dot(x_v[...], wk_v[...], preferred_element_type=F32).astype(BF)
    vn_v[...] = jnp.dot(x_v[...], wv_v[...], preferred_element_type=F32).astype(BF)
    knf[...] = kn_v[pl.ds(start, bl), :].astype(F32)
    vnf[...] = vn_v[pl.ds(start, bl), :].astype(F32)

    ms = yy * 2 + z // 2

    def a_rec(zs):
        return rcopy(wall.at[zs, ld_wq_rows, :], wall.at[zs, ld_wq_rows, :], a_s.at[0], a_r.at[zs],
                     r, zs, ms)

    def x_fwd(zs):
        return rcopy(wall.at[zs, ld_wq_rows, :], wall.at[zs, ld_wq_rows, :], x_s.at[zs], x_r.at[zs],
                     1 - r, z, m)

    other = pl.ds(pl.multiple_of((1 - r) * hr, hr), hr)

    def x_rec(zs):
        return rcopy(wall.at[zs, other, :], wall.at[zs, other, :], x_s.at[zs], x_r.at[zs],
                     1 - r, z, m)

    def qdot(zs):
        cols = pl.ds(pl.multiple_of(zs * de, de), de)
        return jnp.dot(x_v[:, cols], wall[zs], preferred_element_type=F32)

    @pl.when(ms == m)
    def _():
        for tt in range(2):
            for cd in range(2):
                @pl.when((2 * c + tt == z) & (cd == c))
                def _():
                    a_self(tt, cd, tt * 2 + cd).wait()

    @pl.when(ms != m)
    def _():
        rcopy(wall.at[z], wall.at[z], a_s.at[0], a_r.at[z], r, z, my).wait_recv()

    qacc[...] = qdot(z)
    for zs in (near, z2, 3 - z):
        a_rec(zs).wait_recv()
        x_fwd(zs).start()
    for zs in (near, z2, 3 - z):
        x_rec(zs).wait_recv()
        qacc[...] += qdot(zs)
    q_my[...] = qacc[...].astype(BF).reshape(q_my.shape)

    slot = (4 * yy + z) * 2 + c
    for k in range(1, 16):
        p = lax.rem(me + k, 16)
        rcopy(q_my.at[p], q_in.at[slot], c_s.at[k - 1], c_r.at[slot], r, p // 4, p % 4).start()
    q_in[slot] = q_my[me]

    w_z(1).start()
    w_y(1).start()
    w_pass_z(0)

    for k in range(1, 16):
        s_ = lax.rem(slot + k, 16)
        rcopy(q_in.at[s_], q_in.at[s_], c_s.at[k - 1], c_r.at[s_], r, z, m).wait_recv()
    qf[...] = q_in[...].astype(F32).reshape(qf.shape)

    lane = lax.broadcasted_iota(jnp.int32, (nh, t), 1)

    def query(b):
        return jnp.concatenate([qf[pl.ds(b, nh, stride=2 * bl), :],
                                qf[pl.ds(b + bl, nh, stride=2 * bl), :]], axis=1)

    def scores(b):
        return lax.dot_general(query(b).astype(BF), k_v[b], (((1,), (1,)), ((), ())),
                               preferred_element_type=F32) * scale

    def weights(b, s):
        s = jnp.where(lane < lens[start + b], s, -jnp.inf)
        sn = jnp.sum(query(b) * knf[pl.ds(b, 1), :], axis=1, keepdims=True) * scale
        top = jnp.maximum(jnp.max(s, axis=1, keepdims=True), sn)
        p = jnp.exp(s - top)
        pn = jnp.exp(sn - top)
        return p.astype(BF), pn, jnp.sum(p, axis=1, keepdims=True) + pn

    def values(b, bb, p, pn, l):
        acc = jnp.dot(p, v_v[b], preferred_element_type=F32)
        o = (acc + pn.astype(BF).astype(F32) * vnf[pl.ds(b, 1), :]) / l
        of[0, pl.ds(bb, nh, stride=nb), :] = o[:, :half]
        of[1, pl.ds(bb, nh, stride=nb), :] = o[:, half:]

    def attend(base):
        s, p = {}, {}
        for i in range(nb + 2 * LAG):
            if i < nb:
                s[i] = scores(base + i)
            if LAG <= i < nb + LAG:
                p[i - LAG] = weights(base + i - LAG, s.pop(i - LAG))
            if i >= 2 * LAG:
                values(base + i - 2 * LAG, i - 2 * LAG, *p.pop(i - 2 * LAG))

    pair = 2 * (z // 2)
    pos = z % 2
    og = pos * 2 + c

    def o_send(n, k):
        return rcopy(o_in.at[n, og], o_in.at[n, og], o_s.at[n, k], o_r.at[n, og],
                     r, z if k == 0 else near, my if k == 0 else m)

    ng = (1 - pos) * 2 + c

    def o_pass(n):
        return rcopy(o_in.at[n, ng], o_in.at[n, ng], o_s.at[n, 2], o_r.at[n, ng], r, z, my)

    def o_rec(n, g):
        return rcopy(o_in.at[n, g], o_in.at[n, g], o_s.at[n, 0], o_r.at[n, g], r, near, m)

    def o_mid(n):
        o_rec(n, ng).wait_recv()
        o_pass(n).start()

    def blk(n, zs, ms_):
        cols = pl.ds(pl.multiple_of((zs % 2 + 2 * (ms_ % 2)) * de, de), de)
        return y_v.at[pl.ds(2 * (zs // 2), 2), pl.ds(2 * (ms_ // 2), 2), pl.ds(n * nb, nb), cols]

    others = (near, z2, 3 - z)

    def yz_send(n, k):
        return rcopy(blk(n, z, m), blk(n, z, m), yz_s.at[n, k], yz_r.at[n, z], r, others[k], m)

    def yz_rec(n, zs):
        return rcopy(blk(n, zs, m), blk(n, zs, m), yz_s.at[n, 0], yz_r.at[n, zs], r, near, m)

    def yy_send(n, zs):
        return rcopy(blk(n, zs, m), blk(n, zs, m), yy_s.at[n, zs], yy_r.at[n, zs], r, z, mx)

    def yy_rec(n, zs):
        return rcopy(blk(n, zs, mx), blk(n, zs, mx), yy_s.at[n, zs], yy_r.at[n, zs], r, z, mx)

    md = (1 - yy) * 2 + 1 - c

    def yd_send(n, zs, hop):
        ms_ = mx if hop else m
        return rcopy(blk(n, zs, ms_), blk(n, zs, ms_), yd_s.at[n, hop, zs], yd_r.at[n, hop, zs],
                     r, z, my)

    def yd_rec(n, zs, hop):
        ms_ = md if hop else my
        return rcopy(blk(n, zs, ms_), blk(n, zs, ms_), yd_s.at[n, hop, zs], yd_r.at[n, hop, zs],
                     r, z, my)

    def project(n):
        o_rec(n, pos * 2 + 1 - c).wait_recv()
        o_rec(n, (1 - pos) * 2 + 1 - c).wait_recv()
        ob = [o_in[n, g].astype(F32) for g in range(4)]
        acc = jnp.zeros((4 * nb, de), F32)
        for h in range(nh):
            lhs = jnp.concatenate([ob[g][h * nb:(h + 1) * nb] for g in range(4)], axis=0).astype(BF)
            acc = acc + jnp.dot(lhs, wo_v[h // 2, (h % 2) * dh:(h % 2 + 1) * dh, :],
                                preferred_element_type=F32)
        cols = pl.ds(pl.multiple_of((z % 2 + 2 * c) * de, de), de)
        for g in range(4):
            zz = pair + g // 2
            mm = 2 * yy + g % 2
            xr = x_v[pl.ds(pl.multiple_of((zz * 4 + mm) * bl, bl), bl), cols].astype(F32)
            yb = xr[n * nb:(n + 1) * nb] + acc[g * nb:(g + 1) * nb]
            y_v[zz, mm, n * nb:(n + 1) * nb, cols] = yb.astype(BF)
        for k in (2, 1, 0):
            yz_send(n, k).start()
        yy_send(n, z).start()
        yd_send(n, z, 0).start()

    def drain_z(n):
        for zs in others:
            yz_rec(n, zs).wait_recv()
            yy_send(n, zs).start()
            yd_send(n, zs, 0).start()

    def drain_y(n):
        for zs in (z,) + others:
            yy_rec(n, zs).wait_recv()
            yd_send(n, zs, 1).start()

    for n in range(NB):
        for i in range(n * nb // CHUNK, (n + 1) * nb // CHUNK):
            kcp[i].wait()
            vcp[i].wait()
        attend(n * nb)
        o_in[n, og] = jnp.concatenate([of[0], of[1]], axis=1).astype(BF)
        o_send(n, 1).start()
        o_send(n, 0).start()
        if n == 0:
            w_pass_y(0)
            w_pass_z(1)
        else:
            o_mid(n - 1)
        if n == 2:
            w_pass_y(1)

    w_wait()
    for n in range(NB - 1):
        project(n)
    o_mid(NB - 1)
    drain_z(0)
    project(NB - 1)
    for n in range(1, NB):
        drain_z(n)
        drain_y(n - 1)
    drain_y(NB - 1)
    for n in range(NB):
        for hop in range(2):
            for zs in range(4):
                yd_rec(n, zs, hop).wait_recv()

    a_each(lambda d, own: None if own else d.wait_send())
    for k in range(1, 4):
        x_fwd(lax.rem(z + k, 4)).wait_send()
    for k in range(1, 16):
        p = lax.rem(me + k, 16)
        rcopy(q_my.at[p], q_in.at[slot], c_s.at[k - 1], c_r.at[slot], r, p // 4, p % 4).wait_send()
    @pl.when(far)
    def _():
        w_d2d.wait_send()
        for j in range(2):
            for k in range(2):
                w_next(k, j).wait_send()
            for mm in range(4):
                w_twin(mm, j).wait_send()

    for i in range(2):
        w_y(i).wait_send()
        w_z(i).wait_send()
    for n in range(NB):
        for k in range(2):
            o_send(n, k).wait_send()
        o_pass(n).wait_send()
        for k in range(3):
            yz_send(n, k).wait_send()
        for zs in range(4):
            yy_send(n, zs).wait_send()
            yd_send(n, zs, 0).wait_send()
            yd_send(n, zs, 1).wait_send()


def solution(mesh):
    ne = mesh.shape['emb']
    nm = mesh.shape['model']

    def local(x, Wq, Wk, Wv, Wo, Kc, Vc, lengths):
        b, d = x.shape
        t, dh = Kc.shape[1:]
        de = Wq.shape[0]
        bl = b // (ne * nm)
        nb = bl // NB
        nh = 8
        hbm = pl.BlockSpec(memory_space=pl.ANY)
        vmem = pl.BlockSpec(memory_space=pltpu.VMEM)
        dma = pltpu.SemaphoreType.DMA
        y, kn, vn = pl.pallas_call(
            _kernel,
            out_shape=(pltpu.VMEM((ne, nm, bl, d), BF), pltpu.VMEM((b, dh), BF),
                       pltpu.VMEM((b, dh), BF)),
            in_specs=[hbm] * 7 + [pl.BlockSpec(memory_space=pltpu.SMEM)],
            out_specs=(vmem, vmem, vmem),
            scratch_shapes=[
                pltpu.VMEM((b, d), BF), pltpu.VMEM(Wq.shape, BF), pltpu.VMEM((ne, de, dh // 2), BF),
                pltpu.VMEM(Wk.shape, BF), pltpu.VMEM(Wv.shape, BF), pltpu.VMEM(Wo.shape, BF),
                pltpu.VMEM((nm,) + Wo.shape, BF),
                pltpu.VMEM((bl, t, dh), BF), pltpu.VMEM((bl, t, dh), BF),
                pltpu.VMEM((bl, dh), F32), pltpu.VMEM((bl, dh), F32),
                pltpu.VMEM((b, dh // 2), F32),
                pltpu.VMEM((16, bl, dh // 2), BF), pltpu.VMEM((16, bl, dh // 2), BF),
                pltpu.VMEM((16 * bl, dh // 2), F32),
                pltpu.VMEM((2, nh * nb, dh // 2), F32),
                pltpu.VMEM((NB, 4, nh * nb, dh), BF),
                dma((6,)), dma((bl // CHUNK,)), dma((bl // CHUNK,)),
                dma((4,)), dma((4,)), dma((4,)), dma((4,)), dma((15,)), dma((16,)),
                dma((1,)), dma((1,)), dma((2,)), dma((2,)), dma((2, 2)), dma((4, 2)),
                dma((4, 2)), dma((4, 2)),
                dma((NB, 3)), dma((NB, 4)), dma((NB, 3)), dma((NB, 4)),
                dma((NB, 4)), dma((NB, 4)), dma((NB, 2, 4)), dma((NB, 2, 4)),
            ],
            compiler_params=pltpu.CompilerParams(
                collective_id=0, has_side_effects=True, vmem_limit_bytes=VMEM_LIMIT),
        )(x, Wq, Wk, Wv, Wo, Kc, Vc, lengths)
        return y.reshape(b, d), kn, vn

    in_specs = (P('rep', None), P('emb', 'model'), P(), P(), P('model', 'emb'),
                P('rep', None, None), P('rep', None, None), P('rep'))
    out_specs = (P('rep', None), P('rep', None), P('rep', None))
    return jax.shard_map(local, mesh=mesh, in_specs=in_specs, out_specs=out_specs, check_vma=False)
```

```python
import functools

import jax
import jax.numpy as jnp
from jax import lax
from jax.experimental import pallas as pl
from jax.experimental.pallas import tpu as pltpu
from jax.sharding import PartitionSpec as P

BF = jnp.bfloat16
F32 = jnp.float32
NB = 4
J0 = 96
LAG = 2
VMEM_LIMIT = 54 * 1024 * 1024
CHUNK = 8


def _kernel(x_h, wq_h, wk_h, wv_h, wo_h, kc_h, vc_h, lens,
            y_v, kn_v, vn_v,
            x_v, wq_v, wall, wk_v, wv_v, wst, wo_v, k_v, v_v, knf, vnf,
            qacc, q_my, q_in, qf, of, o_in,
            lsem, ksem, vsem,
            a_s, a_r, x_s, x_r, c_s, c_r, w1_s, w1_r, w2_s, w3_s, wn_s, wt_s, wn_r, wt_r,
            o_s, o_r, yz_s, yz_r, yy_s, yy_r, yd_s, yd_r):
    r = lax.axis_index('rep')
    z = lax.axis_index('emb')
    m = lax.axis_index('model')
    yy = m // 2
    c = m % 2
    my = yy * 2 + 1 - c
    mx = (1 - yy) * 2 + c
    near = z + 1 - 2 * (z % 2)
    z2 = lax.rem(z + 2, 4)
    me = z * 4 + m
    bl = k_v.shape[0]
    nb = bl // NB
    t = k_v.shape[1]
    dh = k_v.shape[2]
    nh = 8
    half = dh // 2
    de = wq_v.shape[0]
    hr = de // 2
    start = pl.multiple_of(me * bl, bl)
    scale = dh ** -0.5

    def rcopy(src, dst, ss, rs, rr, zz, mm):
        return pltpu.make_async_remote_copy(
            src_ref=src, dst_ref=dst, send_sem=ss, recv_sem=rs,
            device_id=(rr, zz, mm), device_id_type=pl.DeviceIdType.MESH)

    ld_wq = pltpu.make_async_copy(wq_h, wq_v, lsem.at[0])
    ld_x = pltpu.make_async_copy(x_h, x_v, lsem.at[1])
    ld_wk = pltpu.make_async_copy(wk_h, wk_v, lsem.at[2])
    ld_wv = pltpu.make_async_copy(wv_h, wv_v, lsem.at[3])
    ld_wo = pltpu.make_async_copy(wo_h, wst, lsem.at[4])
    ld_wq.start()
    ld_x.start()
    ld_wk.start()
    ld_wv.start()
    ld_wo.start()
    kcp, vcp = [], []
    for i in range(bl // CHUNK):
        src = pl.ds(start + i * CHUNK, CHUNK)
        dst = pl.ds(i * CHUNK, CHUNK)
        kcp.append(pltpu.make_async_copy(kc_h.at[src], k_v.at[dst], ksem.at[i]))
        vcp.append(pltpu.make_async_copy(vc_h.at[src], v_v.at[dst], vsem.at[i]))

    barrier = pltpu.get_barrier_semaphore()
    for k in range(1, 16):
        p = lax.rem(me + k, 16)
        pl.semaphore_signal(barrier, inc=1, device_id=(r, p // 4, p % 4),
                            device_id_type=pl.DeviceIdType.MESH)
    pl.semaphore_signal(barrier, inc=1, device_id=(1 - r, z, m),
                        device_id_type=pl.DeviceIdType.MESH)
    pl.semaphore_wait(barrier, 16)

    ld_wq.wait()
    ld_wq_rows = pl.ds(pl.multiple_of(r * hr, hr), hr)

    def a_half(tt, cd, i):
        zd = 2 * c + tt
        cols = pl.ds(tt * dh + cd * half, half)
        return rcopy(wq_v.at[ld_wq_rows, cols], wall.at[z, ld_wq_rows, :], a_s.at[i], a_r.at[z],
                     r, zd, yy * 2 + cd)

    def a_full(tt, cd, i):
        cols = pl.ds(tt * dh + cd * half, half)
        return rcopy(wq_v.at[:, cols], wall.at[z], a_s.at[i], a_r.at[z],
                     r, z, yy * 2 + cd)

    def a_self(tt, cd, i):
        cols = pl.ds(tt * dh + cd * half, half)
        return pltpu.make_async_copy(wq_v.at[:, cols], wall.at[z], a_s.at[i])

    def a_each(fn):
        for first in range(2):
            @pl.when(z % 2 == first)
            def _():
                for tt in (first, 1 - first):
                    for cd in range(2):
                        i = tt * 2 + cd
                        zd = 2 * c + tt

                        @pl.when(zd != z)
                        def _():
                            fn(a_half(tt, cd, i), False)

                        @pl.when((zd == z) & (c != cd))
                        def _():
                            fn(a_full(tt, cd, i), False)

                        @pl.when((zd == z) & (c == cd))
                        def _():
                            fn(a_self(tt, cd, i), True)

    a_each(lambda d, own: d.start())

    far = c != z % 2
    ld_wo.wait()
    w_own = pltpu.make_async_copy(wst, wo_v.at[m], lsem.at[5])
    w_d2d = rcopy(wst, wo_v.at[m], w1_s.at[0], w1_r.at[0], r, z, my)

    def w_y(i):
        rows = pl.ds(i * hr, hr)
        return rcopy(wst.at[rows, :], wo_v.at[m, rows, :], w2_s.at[i], wn_r.at[m, i],
                     r, z, (1 - yy) * 2 + z % 2)

    def w_rows(g, j):
        return pl.ds(pl.multiple_of(g * hr + j * J0, 16), hr - J0 if j else J0)

    def w_z(j):
        return rcopy(wst.at[w_rows(r, j), :], wo_v.at[m, w_rows(r, j), :], w3_s.at[j], wn_r.at[m, j],
                     r, near, yy * 2 + z % 2)

    def w_half(mm, j):
        return wo_v.at[mm, w_rows(r, j), :]

    def w_next(k, j):
        mm = 2 * yy + k
        return rcopy(w_half(mm, j), w_half(mm, j), wn_s.at[k, j], wn_r.at[mm, j], r, z, mx)

    def w_twin(mm, j):
        return rcopy(w_half(mm, j), w_half(mm, j), wt_s.at[mm, j], wt_r.at[mm, j], 1 - r, z, m)

    def w_arrived(mm, j):
        return rcopy(w_half(mm, j), w_half(mm, j), wt_s.at[mm, j], wn_r.at[mm, j], r, z, mx)

    def w_pass_z(j):
        @pl.when(far)
        def _():
            for k in range(2):
                w_arrived(2 * yy + k, j).wait_recv()
                w_next(k, j).start()
                w_twin(2 * yy + k, j).start()

    def w_pass_y(j):
        @pl.when(far)
        def _():
            for k in range(2):
                w_arrived(2 * (1 - yy) + k, j).wait_recv()
                w_twin(2 * (1 - yy) + k, j).start()

    def w_wait():
        @pl.when(far)
        def _():
            for mm in range(4):
                for j in range(2):
                    part = wo_v.at[mm, w_rows(1 - r, j), :]
                    rcopy(part, part, wt_s.at[mm, j], wt_r.at[mm, j], 1 - r, z, m).wait_recv()

        @pl.when(~far)
        def _():
            w_own.wait()
            rcopy(wst, wo_v.at[my], w1_s.at[0], w1_r.at[0], r, z, my).wait_recv()
            for k in range(2):
                for i in range(2):
                    part = wo_v.at[2 * (1 - yy) + k, pl.ds(i * hr, hr), :]
                    rcopy(part, part, w2_s.at[i], wn_r.at[2 * (1 - yy) + k, i], r, z, mx).wait_recv()

    @pl.when(far)
    def _():
        w_d2d.start()

    @pl.when(~far)
    def _():
        w_own.start()

    w_z(0).start()
    w_y(0).start()

    ld_x.wait()
    ld_wk.wait()
    ld_wv.wait()
    for i in range(bl // CHUNK):
        kcp[i].start()
        vcp[i].start()
    kn_v[...] = jnp.dot(x_v[...], wk_v[...], preferred_element_type=F32).astype(BF)
    vn_v[...] = jnp.dot(x_v[...], wv_v[...], preferred_element_type=F32).astype(BF)
    knf[...] = kn_v[pl.ds(start, bl), :].astype(F32)
    vnf[...] = vn_v[pl.ds(start, bl), :].astype(F32)

    ms = yy * 2 + z // 2

    def a_rec(zs):
        return rcopy(wall.at[zs, ld_wq_rows, :], wall.at[zs, ld_wq_rows, :], a_s.at[0], a_r.at[zs],
                     r, zs, ms)

    def x_fwd(zs):
        return rcopy(wall.at[zs, ld_wq_rows, :], wall.at[zs, ld_wq_rows, :], x_s.at[zs], x_r.at[zs],
                     1 - r, z, m)

    other = pl.ds(pl.multiple_of((1 - r) * hr, hr), hr)

    def x_rec(zs):
        return rcopy(wall.at[zs, other, :], wall.at[zs, other, :], x_s.at[zs], x_r.at[zs],
                     1 - r, z, m)

    def qdot(zs):
        cols = pl.ds(pl.multiple_of(zs * de, de), de)
        return jnp.dot(x_v[:, cols], wall[zs], preferred_element_type=F32)

    @pl.when(ms == m)
    def _():
        for tt in range(2):
            for cd in range(2):
                @pl.when((2 * c + tt == z) & (cd == c))
                def _():
                    a_self(tt, cd, tt * 2 + cd).wait()

    @pl.when(ms != m)
    def _():
        rcopy(wall.at[z], wall.at[z], a_s.at[0], a_r.at[z], r, z, my).wait_recv()

    qacc[...] = qdot(z)
    for zs in (near, z2, 3 - z):
        a_rec(zs).wait_recv()
        x_fwd(zs).start()
    w_z(1).start()
    for zs in (near, z2, 3 - z):
        x_rec(zs).wait_recv()
        qacc[...] += qdot(zs)
    q_my[...] = qacc[...].astype(BF).reshape(q_my.shape)

    slot = (4 * yy + z) * 2 + c
    for k in range(1, 16):
        p = lax.rem(me + k, 16)
        rcopy(q_my.at[p], q_in.at[slot], c_s.at[k - 1], c_r.at[slot], r, p // 4, p % 4).start()
    q_in[slot] = q_my[me]

    w_pass_z(0)
    w_pass_z(1)
    w_y(1).start()

    for k in range(1, 16):
        s_ = lax.rem(slot + k, 16)
        rcopy(q_in.at[s_], q_in.at[s_], c_s.at[k - 1], c_r.at[s_], r, z, m).wait_recv()
    qf[...] = q_in[...].astype(F32).reshape(qf.shape)

    lane = lax.broadcasted_iota(jnp.int32, (nh, t), 1)

    def query(b):
        return jnp.concatenate([qf[pl.ds(b, nh, stride=2 * bl), :],
                                qf[pl.ds(b + bl, nh, stride=2 * bl), :]], axis=1)

    def scores(b):
        return lax.dot_general(query(b).astype(BF), k_v[b], (((1,), (1,)), ((), ())),
                               preferred_element_type=F32) * scale

    def weights(b, s):
        s = jnp.where(lane < lens[start + b], s, -jnp.inf)
        sn = jnp.sum(query(b) * knf[pl.ds(b, 1), :], axis=1, keepdims=True) * scale
        top = jnp.maximum(jnp.max(s, axis=1, keepdims=True), sn)
        p = jnp.exp(s - top)
        pn = jnp.exp(sn - top)
        return p.astype(BF), pn, jnp.sum(p, axis=1, keepdims=True) + pn

    def values(b, bb, p, pn, l):
        acc = jnp.dot(p, v_v[b], preferred_element_type=F32)
        o = (acc + pn.astype(BF).astype(F32) * vnf[pl.ds(b, 1), :]) / l
        of[0, pl.ds(bb, nh, stride=nb), :] = o[:, :half]
        of[1, pl.ds(bb, nh, stride=nb), :] = o[:, half:]

    def attend(base):
        s, p = {}, {}
        for i in range(nb + 2 * LAG):
            if i < nb:
                s[i] = scores(base + i)
            if LAG <= i < nb + LAG:
                p[i - LAG] = weights(base + i - LAG, s.pop(i - LAG))
            if i >= 2 * LAG:
                values(base + i - 2 * LAG, i - 2 * LAG, *p.pop(i - 2 * LAG))

    pos = z // 2
    og = pos * 2 + c

    def o_send(n, k):
        return rcopy(o_in.at[n, og], o_in.at[n, og], o_s.at[n, k], o_r.at[n, og],
                     r, z if k == 0 else z2, my if k == 0 else m)

    ng = (1 - pos) * 2 + c

    def o_pass(n):
        return rcopy(o_in.at[n, ng], o_in.at[n, ng], o_s.at[n, 2], o_r.at[n, ng], r, z, my)

    def o_rec(n, g):
        return rcopy(o_in.at[n, g], o_in.at[n, g], o_s.at[n, 0], o_r.at[n, g], r, z2, m)

    def o_mid(n):
        o_rec(n, ng).wait_recv()
        o_pass(n).start()

    def blk(n, zs, ms_):
        cols = pl.ds(pl.multiple_of((2 * (zs // 2) + ms_ % 2) * de, de), de)
        return y_v.at[:, zs % 2, pl.ds(2 * (ms_ // 2), 2), pl.ds(n * nb, nb), cols]

    others = (near, 2 - z // 2, 3 - 3 * (z // 2))

    def yz_send(n, k):
        return rcopy(blk(n, z, m), blk(n, z, m), yz_s.at[n, k], yz_r.at[n, z], r, others[k], m)

    def yz_rec(n, zs):
        return rcopy(blk(n, zs, m), blk(n, zs, m), yz_s.at[n, 0], yz_r.at[n, zs], r, near, m)

    def yy_send(n, zs):
        return rcopy(blk(n, zs, m), blk(n, zs, m), yy_s.at[n, zs], yy_r.at[n, zs], r, z, mx)

    def yy_rec(n, zs):
        return rcopy(blk(n, zs, mx), blk(n, zs, mx), yy_s.at[n, zs], yy_r.at[n, zs], r, z, mx)

    md = (1 - yy) * 2 + 1 - c

    def yd_send(n, zs, hop):
        ms_ = mx if hop else m
        return rcopy(blk(n, zs, ms_), blk(n, zs, ms_), yd_s.at[n, hop, zs], yd_r.at[n, hop, zs],
                     r, z, my)

    def yd_rec(n, zs, hop):
        ms_ = md if hop else my
        return rcopy(blk(n, zs, ms_), blk(n, zs, ms_), yd_s.at[n, hop, zs], yd_r.at[n, hop, zs],
                     r, z, my)

    def project(n):
        o_rec(n, pos * 2 + 1 - c).wait_recv()
        o_rec(n, (1 - pos) * 2 + 1 - c).wait_recv()
        ob = [o_in[n, g].astype(F32) for g in range(4)]
        acc = jnp.zeros((4 * nb, de), F32)
        for h in range(nh):
            lhs = jnp.concatenate([ob[g][h * nb:(h + 1) * nb] for g in range(4)], axis=0).astype(BF)
            acc = acc + jnp.dot(lhs, wo_v[h // 2, (h % 2) * dh:(h % 2 + 1) * dh, :],
                                preferred_element_type=F32)
        cols = pl.ds(pl.multiple_of((2 * (z // 2) + c) * de, de), de)
        for g in range(4):
            mm = 2 * yy + g % 2
            row = ((z % 2 + 2 * (g // 2)) * 4 + mm) * bl
            xr = x_v[pl.ds(pl.multiple_of(row, bl), bl), cols].astype(F32)
            yb = xr[n * nb:(n + 1) * nb] + acc[g * nb:(g + 1) * nb]
            y_v[g // 2, z % 2, mm, n * nb:(n + 1) * nb, cols] = yb.astype(BF)
        for k in (2, 1, 0):
            yz_send(n, k).start()
        yy_send(n, z).start()
        yd_send(n, z, 0).start()

    def spread(n, zs):
        yy_send(n, zs).start()
        yd_send(n, zs, 0).start()

    def drain_z(n):
        for zs in others:
            yz_rec(n, zs).wait_recv()
            spread(n, zs)

    def drain_y(n):
        for zs in (z,) + others:
            yy_rec(n, zs).wait_recv()
            yd_send(n, zs, 1).start()

    for n in range(NB):
        for i in range(n * nb // CHUNK, (n + 1) * nb // CHUNK):
            kcp[i].wait()
            vcp[i].wait()
        attend(n * nb)
        o_in[n, og] = jnp.concatenate([of[0], of[1]], axis=1).astype(BF)
        o_send(n, 1).start()
        o_send(n, 0).start()
        if n > 1:
            o_mid(n - 2)
        if n < 2:
            w_pass_y(n)

    w_wait()
    project(0)
    project(1)
    o_mid(2)
    project(2)
    o_mid(3)
    project(3)
    drain_z(0)
    drain_z(1)
    drain_y(0)
    drain_z(2)
    drain_y(1)
    drain_z(3)
    drain_y(2)
    drain_y(3)
    for n in range(NB):
        for hop in range(2):
            for zs in range(4):
                yd_rec(n, zs, hop).wait_recv()

    a_each(lambda d, own: None if own else d.wait_send())
    for k in range(1, 4):
        x_fwd(lax.rem(z + k, 4)).wait_send()
    for k in range(1, 16):
        p = lax.rem(me + k, 16)
        rcopy(q_my.at[p], q_in.at[slot], c_s.at[k - 1], c_r.at[slot], r, p // 4, p % 4).wait_send()
    @pl.when(far)
    def _():
        w_d2d.wait_send()
        for j in range(2):
            for k in range(2):
                w_next(k, j).wait_send()
            for mm in range(4):
                w_twin(mm, j).wait_send()

    for i in range(2):
        w_y(i).wait_send()
        w_z(i).wait_send()
    for n in range(NB):
        for k in range(2):
            o_send(n, k).wait_send()
        o_pass(n).wait_send()
        for k in range(3):
            yz_send(n, k).wait_send()
        for zs in range(4):
            yy_send(n, zs).wait_send()
            yd_send(n, zs, 0).wait_send()
            yd_send(n, zs, 1).wait_send()


def solution(mesh):
    ne = mesh.shape['emb']
    nm = mesh.shape['model']

    def local(x, Wq, Wk, Wv, Wo, Kc, Vc, lengths):
        b, d = x.shape
        t, dh = Kc.shape[1:]
        de = Wq.shape[0]
        bl = b // (ne * nm)
        nb = bl // NB
        nh = 8
        hbm = pl.BlockSpec(memory_space=pl.ANY)
        vmem = pl.BlockSpec(memory_space=pltpu.VMEM)
        dma = pltpu.SemaphoreType.DMA
        y, kn, vn = pl.pallas_call(
            _kernel,
            out_shape=(pltpu.VMEM((2, ne // 2, nm, bl, d), BF), pltpu.VMEM((b, dh), BF),
                       pltpu.VMEM((b, dh), BF)),
            in_specs=[hbm] * 7 + [pl.BlockSpec(memory_space=pltpu.SMEM)],
            out_specs=(vmem, vmem, vmem),
            scratch_shapes=[
                pltpu.VMEM((b, d), BF), pltpu.VMEM(Wq.shape, BF), pltpu.VMEM((ne, de, dh // 2), BF),
                pltpu.VMEM(Wk.shape, BF), pltpu.VMEM(Wv.shape, BF), pltpu.VMEM(Wo.shape, BF),
                pltpu.VMEM((nm,) + Wo.shape, BF),
                pltpu.VMEM((bl, t, dh), BF), pltpu.VMEM((bl, t, dh), BF),
                pltpu.VMEM((bl, dh), F32), pltpu.VMEM((bl, dh), F32),
                pltpu.VMEM((b, dh // 2), F32),
                pltpu.VMEM((16, bl, dh // 2), BF), pltpu.VMEM((16, bl, dh // 2), BF),
                pltpu.VMEM((16 * bl, dh // 2), F32),
                pltpu.VMEM((2, nh * nb, dh // 2), F32),
                pltpu.VMEM((NB, 4, nh * nb, dh), BF),
                dma((6,)), dma((bl // CHUNK,)), dma((bl // CHUNK,)),
                dma((4,)), dma((4,)), dma((4,)), dma((4,)), dma((15,)), dma((16,)),
                dma((1,)), dma((1,)), dma((2,)), dma((2,)), dma((2, 2)), dma((4, 2)),
                dma((4, 2)), dma((4, 2)),
                dma((NB, 3)), dma((NB, 4)), dma((NB, 3)), dma((NB, 4)),
                dma((NB, 4)), dma((NB, 4)), dma((NB, 2, 4)), dma((NB, 2, 4)),
            ],
            compiler_params=pltpu.CompilerParams(
                collective_id=0, has_side_effects=True, vmem_limit_bytes=VMEM_LIMIT),
        )(x, Wq, Wk, Wv, Wo, Kc, Vc, lengths)
        return y.reshape(b, d), kn, vn

    in_specs = (P('rep', None), P('emb', 'model'), P(), P(), P('model', 'emb'),
                P('rep', None, None), P('rep', None, None), P('rep'))
    out_specs = (P('rep', None), P('rep', None), P('rep', None))
    return jax.shard_map(local, mesh=mesh, in_specs=in_specs, out_specs=out_specs, check_vma=False)
```

```python
import functools

import jax
import jax.numpy as jnp
from jax import lax
from jax.experimental import pallas as pl
from jax.experimental.pallas import tpu as pltpu
from jax.sharding import PartitionSpec as P

BF = jnp.bfloat16
F32 = jnp.float32
NB = 4
J0 = 96
LAG = 2
VMEM_LIMIT = 54 * 1024 * 1024
CHUNK = 8


def _kernel(x_h, wq_h, wk_h, wv_h, wo_h, kc_h, vc_h, lens,
            y_v, kn_v, vn_v,
            x_v, wq_v, wall, wk_v, wv_v, wst, wo_v, k_v, v_v, knf, vnf,
            qacc, q_my, q_in, qf, of, o_in,
            lsem, ksem, vsem,
            a_s, a_r, x_s, x_r, c_s, c_r, w1_s, w1_r, w2_s, w3_s, wn_s, wt_s, wn_r, wt_r,
            o_s, o_r, yz_s, yz_r, yy_s, yy_r, yd_s, yd_r):
    r = lax.axis_index('rep')
    z = lax.axis_index('emb')
    m = lax.axis_index('model')
    yy = m // 2
    c = m % 2
    my = yy * 2 + 1 - c
    mx = (1 - yy) * 2 + c
    near = z + 1 - 2 * (z % 2)
    z2 = lax.rem(z + 2, 4)
    me = z * 4 + m
    bl = k_v.shape[0]
    nb = bl // NB
    t = k_v.shape[1]
    dh = k_v.shape[2]
    nh = 8
    half = dh // 2
    de = wq_v.shape[0]
    hr = de // 2
    start = pl.multiple_of(me * bl, bl)
    scale = dh ** -0.5

    def rcopy(src, dst, ss, rs, rr, zz, mm):
        return pltpu.make_async_remote_copy(
            src_ref=src, dst_ref=dst, send_sem=ss, recv_sem=rs,
            device_id=(rr, zz, mm), device_id_type=pl.DeviceIdType.MESH)

    ld_wq = pltpu.make_async_copy(wq_h, wq_v, lsem.at[0])
    ld_x = pltpu.make_async_copy(x_h, x_v, lsem.at[1])
    ld_wk = pltpu.make_async_copy(wk_h, wk_v, lsem.at[2])
    ld_wv = pltpu.make_async_copy(wv_h, wv_v, lsem.at[3])
    ld_wo = pltpu.make_async_copy(wo_h, wst, lsem.at[4])
    ld_wq.start()
    ld_x.start()
    ld_wk.start()
    ld_wv.start()
    ld_wo.start()
    kcp, vcp = [], []
    for i in range(bl // CHUNK):
        src = pl.ds(start + i * CHUNK, CHUNK)
        dst = pl.ds(i * CHUNK, CHUNK)
        kcp.append(pltpu.make_async_copy(kc_h.at[src], k_v.at[dst], ksem.at[i]))
        vcp.append(pltpu.make_async_copy(vc_h.at[src], v_v.at[dst], vsem.at[i]))

    barrier = pltpu.get_barrier_semaphore()
    for k in range(1, 16):
        p = lax.rem(me + k, 16)
        pl.semaphore_signal(barrier, inc=1, device_id=(r, p // 4, p % 4),
                            device_id_type=pl.DeviceIdType.MESH)
    pl.semaphore_signal(barrier, inc=1, device_id=(1 - r, z, m),
                        device_id_type=pl.DeviceIdType.MESH)
    pl.semaphore_wait(barrier, 16)

    ld_wq.wait()
    ld_wq_rows = pl.ds(pl.multiple_of(r * hr, hr), hr)

    def a_half(tt, cd, i):
        zd = 2 * c + tt
        cols = pl.ds(tt * dh + cd * half, half)
        return rcopy(wq_v.at[ld_wq_rows, cols], wall.at[z, ld_wq_rows, :], a_s.at[i], a_r.at[z],
                     r, zd, yy * 2 + cd)

    def a_full(tt, cd, i):
        cols = pl.ds(tt * dh + cd * half, half)
        return rcopy(wq_v.at[:, cols], wall.at[z], a_s.at[i], a_r.at[z],
                     r, z, yy * 2 + cd)

    def a_self(tt, cd, i):
        cols = pl.ds(tt * dh + cd * half, half)
        return pltpu.make_async_copy(wq_v.at[:, cols], wall.at[z], a_s.at[i])

    def a_each(fn):
        for first in range(2):
            @pl.when(z % 2 == first)
            def _():
                for tt in (first, 1 - first):
                    for cd in range(2):
                        i = tt * 2 + cd
                        zd = 2 * c + tt

                        @pl.when(zd != z)
                        def _():
                            fn(a_half(tt, cd, i), False)

                        @pl.when((zd == z) & (c != cd))
                        def _():
                            fn(a_full(tt, cd, i), False)

                        @pl.when((zd == z) & (c == cd))
                        def _():
                            fn(a_self(tt, cd, i), True)

    a_each(lambda d, own: d.start())

    far = c != z % 2
    ld_wo.wait()
    w_own = pltpu.make_async_copy(wst, wo_v.at[m], lsem.at[5])
    w_d2d = rcopy(wst, wo_v.at[m], w1_s.at[0], w1_r.at[0], r, z, my)

    def w_y(i):
        rows = pl.ds(i * hr, hr)
        return rcopy(wst.at[rows, :], wo_v.at[m, rows, :], w2_s.at[i], wn_r.at[m, i],
                     r, z, (1 - yy) * 2 + z % 2)

    def w_rows(g, j):
        return pl.ds(pl.multiple_of(g * hr + j * J0, 16), hr - J0 if j else J0)

    def w_z(j):
        return rcopy(wst.at[w_rows(r, j), :], wo_v.at[m, w_rows(r, j), :], w3_s.at[j], wn_r.at[m, j],
                     r, near, yy * 2 + z % 2)

    def w_half(mm, j):
        return wo_v.at[mm, w_rows(r, j), :]

    def w_next(k, j):
        mm = 2 * yy + k
        return rcopy(w_half(mm, j), w_half(mm, j), wn_s.at[k, j], wn_r.at[mm, j], r, z, mx)

    def w_twin(mm, j):
        return rcopy(w_half(mm, j), w_half(mm, j), wt_s.at[mm, j], wt_r.at[mm, j], 1 - r, z, m)

    def w_arrived(mm, j):
        return rcopy(w_half(mm, j), w_half(mm, j), wt_s.at[mm, j], wn_r.at[mm, j], r, z, mx)

    def w_pass_z(j):
        @pl.when(far)
        def _():
            for k in range(2):
                w_arrived(2 * yy + k, j).wait_recv()
                w_next(k, j).start()
                w_twin(2 * yy + k, j).start()

    def w_pass_y(j):
        @pl.when(far)
        def _():
            for k in range(2):
                w_arrived(2 * (1 - yy) + k, j).wait_recv()
                w_twin(2 * (1 - yy) + k, j).start()

    def w_wait():
        @pl.when(far)
        def _():
            for mm in range(4):
                for j in range(2):
                    part = wo_v.at[mm, w_rows(1 - r, j), :]
                    rcopy(part, part, wt_s.at[mm, j], wt_r.at[mm, j], 1 - r, z, m).wait_recv()

        @pl.when(~far)
        def _():
            w_own.wait()
            rcopy(wst, wo_v.at[my], w1_s.at[0], w1_r.at[0], r, z, my).wait_recv()
            for k in range(2):
                for i in range(2):
                    part = wo_v.at[2 * (1 - yy) + k, pl.ds(i * hr, hr), :]
                    rcopy(part, part, w2_s.at[i], wn_r.at[2 * (1 - yy) + k, i], r, z, mx).wait_recv()

    @pl.when(far)
    def _():
        w_d2d.start()

    @pl.when(~far)
    def _():
        w_own.start()

    w_z(0).start()
    w_y(0).start()

    @pl.when(~far)
    def _():
        w_y(1).start()

    ld_x.wait()
    ld_wk.wait()
    ld_wv.wait()
    for i in range(bl // CHUNK):
        kcp[i].start()
        vcp[i].start()
    kn_v[...] = jnp.dot(x_v[...], wk_v[...], preferred_element_type=F32).astype(BF)
    vn_v[...] = jnp.dot(x_v[...], wv_v[...], preferred_element_type=F32).astype(BF)
    knf[...] = kn_v[pl.ds(start, bl), :].astype(F32)
    vnf[...] = vn_v[pl.ds(start, bl), :].astype(F32)

    ms = yy * 2 + z // 2

    def a_rec(zs):
        return rcopy(wall.at[zs, ld_wq_rows, :], wall.at[zs, ld_wq_rows, :], a_s.at[0], a_r.at[zs],
                     r, zs, ms)

    def x_fwd(zs):
        return rcopy(wall.at[zs, ld_wq_rows, :], wall.at[zs, ld_wq_rows, :], x_s.at[zs], x_r.at[zs],
                     1 - r, z, m)

    other = pl.ds(pl.multiple_of((1 - r) * hr, hr), hr)

    def x_rec(zs):
        return rcopy(wall.at[zs, other, :], wall.at[zs, other, :], x_s.at[zs], x_r.at[zs],
                     1 - r, z, m)

    def qdot(zs):
        cols = pl.ds(pl.multiple_of(zs * de, de), de)
        return jnp.dot(x_v[:, cols], wall[zs], preferred_element_type=F32)

    @pl.when(ms == m)
    def _():
        for tt in range(2):
            for cd in range(2):
                @pl.when((2 * c + tt == z) & (cd == c))
                def _():
                    a_self(tt, cd, tt * 2 + cd).wait()

    @pl.when(ms != m)
    def _():
        rcopy(wall.at[z], wall.at[z], a_s.at[0], a_r.at[z], r, z, my).wait_recv()

    qacc[...] = qdot(z)
    for zs in (near, z2, 3 - z):
        a_rec(zs).wait_recv()
        x_fwd(zs).start()
    w_z(1).start()
    w_pass_z(0)
    for zs in (near, z2, 3 - z):
        x_rec(zs).wait_recv()
        qacc[...] += qdot(zs)
    q_my[...] = qacc[...].astype(BF).reshape(q_my.shape)

    slot = (4 * yy + z) * 2 + c
    qh = bl // 2

    def q_copy(hf, k):
        p = lax.rem(me + k, 16)
        rows = pl.ds(hf * qh, qh)
        return rcopy(q_my.at[p, rows, :], q_in.at[slot, rows, :], c_s.at[hf, k - 1], c_r.at[hf, slot],
                     r, p // 4, p % 4)

    for hf in range(2):
        for k in range(1, 16):
            q_copy(hf, k).start()
    q_in[slot] = q_my[me]

    def q_wait(hf):
        rows = pl.ds(hf * qh, qh)
        for k in range(1, 16):
            s_ = lax.rem(slot + k, 16)
            rcopy(q_in.at[s_, rows, :], q_in.at[s_, rows, :], c_s.at[hf, k - 1], c_r.at[hf, s_],
                  r, z, m).wait_recv()
        for s_ in range(16):
            qf[s_ * bl + hf * qh:s_ * bl + (hf + 1) * qh, :] = (
                q_in[s_, hf * qh:(hf + 1) * qh, :].astype(F32))

    w_pass_z(1)

    @pl.when(far)
    def _():
        w_y(1).start()

    w_pass_y(0)

    q_wait(0)

    lane = lax.broadcasted_iota(jnp.int32, (nh, t), 1)

    def query(b):
        return jnp.concatenate([qf[pl.ds(b, nh, stride=2 * bl), :],
                                qf[pl.ds(b + bl, nh, stride=2 * bl), :]], axis=1)

    def scores(b):
        return lax.dot_general(query(b).astype(BF), k_v[b], (((1,), (1,)), ((), ())),
                               preferred_element_type=F32) * scale

    def weights(b, s):
        s = jnp.where(lane < lens[start + b], s, -jnp.inf)
        sn = jnp.sum(query(b) * knf[pl.ds(b, 1), :], axis=1, keepdims=True) * scale
        top = jnp.maximum(jnp.max(s, axis=1, keepdims=True), sn)
        p = jnp.exp(s - top)
        pn = jnp.exp(sn - top)
        return p.astype(BF), pn, jnp.sum(p, axis=1, keepdims=True) + pn

    def values(b, bb, p, pn, l):
        acc = jnp.dot(p, v_v[b], preferred_element_type=F32)
        o = (acc + pn.astype(BF).astype(F32) * vnf[pl.ds(b, 1), :]) / l
        of[0, pl.ds(bb, nh, stride=nb), :] = o[:, :half]
        of[1, pl.ds(bb, nh, stride=nb), :] = o[:, half:]

    pos = z // 2
    og = pos * 2 + c

    def o_send(n, k):
        return rcopy(o_in.at[n, og], o_in.at[n, og], o_s.at[n, k], o_r.at[n, og],
                     r, z if k == 0 else z2, my if k == 0 else m)

    ng = (1 - pos) * 2 + c

    def o_pass(n):
        return rcopy(o_in.at[n, ng], o_in.at[n, ng], o_s.at[n, 2], o_r.at[n, ng], r, z, my)

    def o_rec(n, g):
        return rcopy(o_in.at[n, g], o_in.at[n, g], o_s.at[n, 0], o_r.at[n, g], r, z2, m)

    def o_mid(n):
        o_rec(n, ng).wait_recv()
        o_pass(n).start()

    def blk(n, zs, ms_):
        cols = pl.ds(pl.multiple_of((2 * (zs // 2) + ms_ % 2) * de, de), de)
        return y_v.at[:, zs % 2, pl.ds(2 * (ms_ // 2), 2), pl.ds(n * nb, nb), cols]

    others = (near, 2 - z // 2, 3 - 3 * (z // 2))

    def yz_send(n, k):
        return rcopy(blk(n, z, m), blk(n, z, m), yz_s.at[n, k], yz_r.at[n, z], r, others[k], m)

    inner = (z == 1) | (z == 2)
    ii = lax.rem((z + 1) // 2, 2)
    arrive = (near + ii * (others[1] - near), others[2] + ii * (near - others[2]),
              others[1] + ii * (others[2] - others[1]))

    def yz_pass(n):
        zs = others[1]
        return rcopy(blk(n, zs, m), blk(n, zs, m), yz_s.at[n, 3], yz_r.at[n, zs], r, near, m)

    def yz_rec(n, zs):
        return rcopy(blk(n, zs, m), blk(n, zs, m), yz_s.at[n, 0], yz_r.at[n, zs], r, near, m)

    def yy_send(n, zs):
        return rcopy(blk(n, zs, m), blk(n, zs, m), yy_s.at[n, zs], yy_r.at[n, zs], r, z, mx)

    def yy_rec(n, zs):
        return rcopy(blk(n, zs, mx), blk(n, zs, mx), yy_s.at[n, zs], yy_r.at[n, zs], r, z, mx)

    md = (1 - yy) * 2 + 1 - c

    def yd_send(n, zs, hop):
        ms_ = mx if hop else m
        return rcopy(blk(n, zs, ms_), blk(n, zs, ms_), yd_s.at[n, hop, zs], yd_r.at[n, hop, zs],
                     r, z, my)

    def yd_rec(n, zs, hop):
        ms_ = md if hop else my
        return rcopy(blk(n, zs, ms_), blk(n, zs, ms_), yd_s.at[n, hop, zs], yd_r.at[n, hop, zs],
                     r, z, my)

    def project(n):
        o_rec(n, pos * 2 + 1 - c).wait_recv()
        o_rec(n, (1 - pos) * 2 + 1 - c).wait_recv()
        ob = [o_in[n, g].astype(F32) for g in range(4)]
        lhs = jnp.concatenate(
            [jnp.concatenate([ob[g][h * nb:(h + 1) * nb] for g in range(4)], axis=0).astype(BF)
             for h in range(nh)], axis=1)
        acc = jnp.dot(lhs, wo_v[...].reshape(nh * dh, de), preferred_element_type=F32)
        cols = pl.ds(pl.multiple_of((2 * (z // 2) + c) * de, de), de)
        for g in range(4):
            mm = 2 * yy + g % 2
            row = ((z % 2 + 2 * (g // 2)) * 4 + mm) * bl
            xr = x_v[pl.ds(pl.multiple_of(row, bl), bl), cols].astype(F32)
            yb = xr[n * nb:(n + 1) * nb] + acc[g * nb:(g + 1) * nb]
            y_v[g // 2, z % 2, mm, n * nb:(n + 1) * nb, cols] = yb.astype(BF)
        @pl.when(~inner)
        def _():
            yz_send(n, 2).start()

        yz_send(n, 1).start()
        yz_send(n, 0).start()
        yy_send(n, z).start()
        yd_send(n, z, 0).start()

    def spread(n, zs):
        yy_send(n, zs).start()
        yd_send(n, zs, 0).start()

    def drain_z(n):
        for k, zs in enumerate(arrive):
            yz_rec(n, zs).wait_recv()
            if k == 0:
                @pl.when(inner)
                def _():
                    yz_pass(n).start()
            spread(n, zs)

    def drain_y(n):
        for zs in (z,) + others:
            yy_rec(n, zs).wait_recv()
            yd_send(n, zs, 1).start()

    s, p = {}, {}
    for i in range(bl + 2 * LAG):
        if i < bl:
            if i == qh:
                q_wait(1)
            if i % CHUNK == 0:
                kcp[i // CHUNK].wait()
                vcp[i // CHUNK].wait()
            s[i] = scores(i)
        if LAG <= i < bl + LAG:
            p[i - LAG] = weights(i - LAG, s.pop(i - LAG))
        if i >= 2 * LAG:
            b = i - 2 * LAG
            values(b, b % nb, *p.pop(b))
            if (b + 1) % nb == 0:
                n = b // nb
                o_in[n, og] = jnp.concatenate([of[0], of[1]], axis=1).astype(BF)
                o_send(n, 1).start()
                o_send(n, 0).start()
                if n > 1:
                    o_mid(n - 2)
                if n == 0:
                    w_pass_y(1)

    w_wait()
    project(0)
    project(1)
    o_mid(2)
    project(2)
    o_mid(3)
    project(3)
    drain_z(0)
    drain_z(1)
    drain_z(2)
    drain_z(3)
    drain_y(0)
    drain_y(1)
    drain_y(2)
    drain_y(3)
    for n in range(NB):
        for hop in range(2):
            for zs in range(4):
                yd_rec(n, zs, hop).wait_recv()

    a_each(lambda d, own: None if own else d.wait_send())
    for k in range(1, 4):
        x_fwd(lax.rem(z + k, 4)).wait_send()
    for hf in range(2):
        for k in range(1, 16):
            q_copy(hf, k).wait_send()
    @pl.when(far)
    def _():
        w_d2d.wait_send()
        for j in range(2):
            for k in range(2):
                w_next(k, j).wait_send()
            for mm in range(4):
                w_twin(mm, j).wait_send()

    for i in range(2):
        w_y(i).wait_send()
        w_z(i).wait_send()
    for n in range(NB):
        for k in range(2):
            o_send(n, k).wait_send()
        o_pass(n).wait_send()
        yz_send(n, 0).wait_send()
        yz_send(n, 1).wait_send()

        @pl.when(~inner)
        def _():
            yz_send(n, 2).wait_send()

        @pl.when(inner)
        def _():
            yz_pass(n).wait_send()

        for zs in range(4):
            yy_send(n, zs).wait_send()
            yd_send(n, zs, 0).wait_send()
            yd_send(n, zs, 1).wait_send()


def _store(y_v, kn_v, vn_v, y_h, kn_h, vn_h, sem):
    copies = [pltpu.make_async_copy(y_v, y_h, sem.at[0]),
              pltpu.make_async_copy(kn_v, kn_h, sem.at[1]),
              pltpu.make_async_copy(vn_v, vn_h, sem.at[2])]
    for copy in copies:
        copy.start()
    for copy in copies:
        copy.wait()


def solution(mesh):
    ne = mesh.shape['emb']
    nm = mesh.shape['model']

    def local(x, Wq, Wk, Wv, Wo, Kc, Vc, lengths):
        b, d = x.shape
        t, dh = Kc.shape[1:]
        de = Wq.shape[0]
        bl = b // (ne * nm)
        nb = bl // NB
        nh = 8
        hbm = pl.BlockSpec(memory_space=pl.ANY)
        vmem = pl.BlockSpec(memory_space=pltpu.VMEM)
        dma = pltpu.SemaphoreType.DMA
        y, kn, vn = pl.pallas_call(
            _kernel,
            out_shape=(pltpu.VMEM((2, ne // 2, nm, bl, d), BF), pltpu.VMEM((b, dh), BF),
                       pltpu.VMEM((b, dh), BF)),
            in_specs=[hbm] * 7 + [pl.BlockSpec(memory_space=pltpu.SMEM)],
            out_specs=(vmem, vmem, vmem),
            scratch_shapes=[
                pltpu.VMEM((b, d), BF), pltpu.VMEM(Wq.shape, BF), pltpu.VMEM((ne, de, dh // 2), BF),
                pltpu.VMEM(Wk.shape, BF), pltpu.VMEM(Wv.shape, BF), pltpu.VMEM(Wo.shape, BF),
                pltpu.VMEM((nm,) + Wo.shape, BF),
                pltpu.VMEM((bl, t, dh), BF), pltpu.VMEM((bl, t, dh), BF),
                pltpu.VMEM((bl, dh), F32), pltpu.VMEM((bl, dh), F32),
                pltpu.VMEM((b, dh // 2), F32),
                pltpu.VMEM((16, bl, dh // 2), BF), pltpu.VMEM((16, bl, dh // 2), BF),
                pltpu.VMEM((16 * bl, dh // 2), F32),
                pltpu.VMEM((2, nh * nb, dh // 2), F32),
                pltpu.VMEM((NB, 4, nh * nb, dh), BF),
                dma((6,)), dma((bl // CHUNK,)), dma((bl // CHUNK,)),
                dma((4,)), dma((4,)), dma((4,)), dma((4,)), dma((2, 15)), dma((2, 16)),
                dma((1,)), dma((1,)), dma((2,)), dma((2,)), dma((2, 2)), dma((4, 2)),
                dma((4, 2)), dma((4, 2)),
                dma((NB, 3)), dma((NB, 4)), dma((NB, 4)), dma((NB, 4)),
                dma((NB, 4)), dma((NB, 4)), dma((NB, 2, 4)), dma((NB, 2, 4)),
            ],
            compiler_params=pltpu.CompilerParams(
                collective_id=0, has_side_effects=True, vmem_limit_bytes=VMEM_LIMIT),
        )(x, Wq, Wk, Wv, Wo, Kc, Vc, lengths)
        y, kn, vn = (pltpu.with_memory_space_constraint(a, pltpu.VMEM) for a in (y.reshape(b, d), kn, vn))
        return pl.pallas_call(
            _store,
            out_shape=(jax.ShapeDtypeStruct((b, d), BF), jax.ShapeDtypeStruct((b, dh), BF),
                       jax.ShapeDtypeStruct((b, dh), BF)),
            in_specs=[vmem] * 3,
            out_specs=(hbm, hbm, hbm),
            scratch_shapes=[dma((3,))],
        )(y, kn, vn)

    in_specs = (P('rep', None), P('emb', 'model'), P(), P(), P('model', 'emb'),
                P('rep', None, None), P('rep', None, None), P('rep'))
    out_specs = (P('rep', None), P('rep', None), P('rep', None))
    return jax.shard_map(local, mesh=mesh, in_specs=in_specs, out_specs=out_specs, check_vma=False)
```

```python
import functools

import jax
import jax.numpy as jnp
from jax import lax
from jax.experimental import pallas as pl
from jax.experimental.pallas import tpu as pltpu
from jax.sharding import PartitionSpec as P

BF = jnp.bfloat16
F32 = jnp.float32
NB = 4
J0 = 96
LAG = 2
VMEM_LIMIT = 54 * 1024 * 1024
CHUNK = 8


def _kernel(x_h, wq_h, wk_h, wv_h, wo_h, kc_h, vc_h, lens,
            y_v, kn_v, vn_v,
            x_v, wq_v, wall, wk_v, wv_v, wst, wo_v, k_v, v_v, knf, vnf,
            qacc, q_my, q_in, qf, of, o_in,
            lsem, ksem, vsem,
            a_s, a_r, x_s, x_r, c_s, c_r, w1_s, w1_r, w2_s, w3_s, wn_s, wt_s, wn_r, wt_r,
            o_s, o_r, yz_s, yz_r, yy_s, yy_r, yd_s, yd_r):
    r = lax.axis_index('rep')
    z = lax.axis_index('emb')
    m = lax.axis_index('model')
    yy = m // 2
    c = m % 2
    my = yy * 2 + 1 - c
    mx = (1 - yy) * 2 + c
    near = z + 1 - 2 * (z % 2)
    z2 = lax.rem(z + 2, 4)
    me = z * 4 + m
    bl = k_v.shape[0]
    nb = bl // NB
    t = k_v.shape[1]
    dh = k_v.shape[2]
    nh = 8
    half = dh // 2
    de = wq_v.shape[0]
    hr = de // 2
    start = pl.multiple_of(me * bl, bl)
    scale = dh ** -0.5

    def rcopy(src, dst, ss, rs, rr, zz, mm):
        return pltpu.make_async_remote_copy(
            src_ref=src, dst_ref=dst, send_sem=ss, recv_sem=rs,
            device_id=(rr, zz, mm), device_id_type=pl.DeviceIdType.MESH)

    ld_wq = pltpu.make_async_copy(wq_h, wq_v, lsem.at[0])
    ld_x = pltpu.make_async_copy(x_h, x_v, lsem.at[1])
    ld_wk = pltpu.make_async_copy(wk_h, wk_v, lsem.at[2])
    ld_wv = pltpu.make_async_copy(wv_h, wv_v, lsem.at[3])
    ld_wo = pltpu.make_async_copy(wo_h, wst, lsem.at[4])
    ld_wq.start()
    ld_x.start()
    ld_wk.start()
    ld_wv.start()
    ld_wo.start()
    kcp, vcp = [], []
    for i in range(bl // CHUNK):
        src = pl.ds(start + i * CHUNK, CHUNK)
        dst = pl.ds(i * CHUNK, CHUNK)
        kcp.append(pltpu.make_async_copy(kc_h.at[src], k_v.at[dst], ksem.at[i]))
        vcp.append(pltpu.make_async_copy(vc_h.at[src], v_v.at[dst], vsem.at[i]))

    barrier = pltpu.get_barrier_semaphore()
    for k in range(1, 16):
        p = lax.rem(me + k, 16)
        pl.semaphore_signal(barrier, inc=1, device_id=(r, p // 4, p % 4),
                            device_id_type=pl.DeviceIdType.MESH)
    pl.semaphore_signal(barrier, inc=1, device_id=(1 - r, z, m),
                        device_id_type=pl.DeviceIdType.MESH)
    pl.semaphore_wait(barrier, 16)

    ld_wq.wait()
    hq = hr // 2

    def quarter(g, j):
        return pl.ds(pl.multiple_of(g * hr + j * hq, hq), hq)

    def a_half(tt, cd, i, j):
        zd = 2 * c + tt
        cols = pl.ds(tt * dh + cd * half, half)
        rows = quarter(r, j)
        return rcopy(wq_v.at[rows, cols], wall.at[z, rows, :], a_s.at[i, j], a_r.at[z, j],
                     r, zd, yy * 2 + cd)

    def a_full(tt, cd, i):
        cols = pl.ds(tt * dh + cd * half, half)
        return rcopy(wq_v.at[:, cols], wall.at[z], a_s.at[i, 0], a_r.at[z, 0],
                     r, z, yy * 2 + cd)

    def a_self(tt, cd, i):
        cols = pl.ds(tt * dh + cd * half, half)
        return pltpu.make_async_copy(wq_v.at[:, cols], wall.at[z], a_s.at[i, 0])

    def a_each(fn):
        for first in range(2):
            @pl.when(z % 2 == first)
            def _():
                for tt in (first, 1 - first):
                    for cd in range(2):
                        i = tt * 2 + cd
                        zd = 2 * c + tt

                        @pl.when(zd != z)
                        def _():
                            fn(a_half(tt, cd, i, 0), False)
                            fn(a_half(tt, cd, i, 1), False)

                        @pl.when((zd == z) & (c != cd))
                        def _():
                            fn(a_full(tt, cd, i), False)

                        @pl.when((zd == z) & (c == cd))
                        def _():
                            fn(a_self(tt, cd, i), True)

    a_each(lambda d, own: d.start())

    far = c != z % 2
    ld_wo.wait()
    w_own = pltpu.make_async_copy(wst, wo_v.at[m], lsem.at[5])
    w_d2d = rcopy(wst, wo_v.at[m], w1_s.at[0], w1_r.at[0], r, z, my)

    def w_y(i):
        rows = pl.ds(i * hr, hr)
        return rcopy(wst.at[rows, :], wo_v.at[m, rows, :], w2_s.at[i], wn_r.at[m, i],
                     r, z, (1 - yy) * 2 + z % 2)

    def w_rows(g, j):
        return pl.ds(pl.multiple_of(g * hr + j * J0, 16), hr - J0 if j else J0)

    def w_z(j):
        return rcopy(wst.at[w_rows(r, j), :], wo_v.at[m, w_rows(r, j), :], w3_s.at[j], wn_r.at[m, j],
                     r, near, yy * 2 + z % 2)

    def w_half(mm, j):
        return wo_v.at[mm, w_rows(r, j), :]

    def w_next(k, j):
        mm = 2 * yy + k
        return rcopy(w_half(mm, j), w_half(mm, j), wn_s.at[k, j], wn_r.at[mm, j], r, z, mx)

    def w_twin(mm, j):
        return rcopy(w_half(mm, j), w_half(mm, j), wt_s.at[mm, j], wt_r.at[mm, j], 1 - r, z, m)

    def w_arrived(mm, j):
        return rcopy(w_half(mm, j), w_half(mm, j), wt_s.at[mm, j], wn_r.at[mm, j], r, z, mx)

    def w_pass_z(j):
        @pl.when(far)
        def _():
            for k in range(2):
                w_arrived(2 * yy + k, j).wait_recv()
                w_next(k, j).start()
                w_twin(2 * yy + k, j).start()

    def w_pass_y(j):
        @pl.when(far)
        def _():
            for k in range(2):
                w_arrived(2 * (1 - yy) + k, j).wait_recv()
                w_twin(2 * (1 - yy) + k, j).start()

    def w_wait():
        @pl.when(far)
        def _():
            for mm in range(4):
                for j in range(2):
                    part = wo_v.at[mm, w_rows(1 - r, j), :]
                    rcopy(part, part, wt_s.at[mm, j], wt_r.at[mm, j], 1 - r, z, m).wait_recv()

        @pl.when(~far)
        def _():
            w_own.wait()
            rcopy(wst, wo_v.at[my], w1_s.at[0], w1_r.at[0], r, z, my).wait_recv()
            for k in range(2):
                for i in range(2):
                    part = wo_v.at[2 * (1 - yy) + k, pl.ds(i * hr, hr), :]
                    rcopy(part, part, w2_s.at[i], wn_r.at[2 * (1 - yy) + k, i], r, z, mx).wait_recv()

    @pl.when(far)
    def _():
        w_d2d.start()

    @pl.when(~far)
    def _():
        w_own.start()

    w_y(0).start()

    @pl.when(~far)
    def _():
        w_y(1).start()

    ld_x.wait()
    ld_wk.wait()
    ld_wv.wait()
    for i in range(bl // CHUNK):
        kcp[i].start()
        vcp[i].start()
    kn_v[...] = jnp.dot(x_v[...], wk_v[...], preferred_element_type=F32).astype(BF)
    vn_v[...] = jnp.dot(x_v[...], wv_v[...], preferred_element_type=F32).astype(BF)
    knf[...] = kn_v[pl.ds(start, bl), :].astype(F32)
    vnf[...] = vn_v[pl.ds(start, bl), :].astype(F32)

    ms = yy * 2 + z // 2

    def a_rec(zs, j):
        part = wall.at[zs, quarter(r, j), :]
        return rcopy(part, part, a_s.at[0, 0], a_r.at[zs, j], r, zs, ms)

    def x_fwd(zs, j):
        part = wall.at[zs, quarter(r, j), :]
        return rcopy(part, part, x_s.at[zs, j], x_r.at[zs, j], 1 - r, z, m)

    def x_rec(zs, j):
        part = wall.at[zs, quarter(1 - r, j), :]
        return rcopy(part, part, x_s.at[zs, j], x_r.at[zs, j], 1 - r, z, m)

    def qdot(zs):
        cols = pl.ds(pl.multiple_of(zs * de, de), de)
        return jnp.dot(x_v[:, cols], wall[zs], preferred_element_type=F32)

    @pl.when(ms == m)
    def _():
        for tt in range(2):
            for cd in range(2):
                @pl.when((2 * c + tt == z) & (cd == c))
                def _():
                    a_self(tt, cd, tt * 2 + cd).wait()

    @pl.when(ms != m)
    def _():
        rcopy(wall.at[z], wall.at[z], a_s.at[0, 0], a_r.at[z, 0], r, z, my).wait_recv()

    qacc[...] = qdot(z)
    for zs in (near, z2, 3 - z):
        for j in range(2):
            a_rec(zs, j).wait_recv()
            x_fwd(zs, j).start()
        if zs is near:
            w_z(0).start()
    w_z(1).start()
    w_pass_z(0)
    for zs in (near, z2, 3 - z):
        x_rec(zs, 0).wait_recv()
        x_rec(zs, 1).wait_recv()
        qacc[...] += qdot(zs)
    q_my[...] = qacc[...].astype(BF).reshape(q_my.shape)

    slot = (4 * yy + z) * 2 + c
    qh = bl // 2

    def q_copy(hf, k):
        p = lax.rem(me + k, 16)
        rows = pl.ds(hf * qh, qh)
        return rcopy(q_my.at[p, rows, :], q_in.at[slot, rows, :], c_s.at[hf, k - 1], c_r.at[hf, slot],
                     r, p // 4, p % 4)

    for hf in range(2):
        for k in range(1, 16):
            q_copy(hf, k).start()
    q_in[slot] = q_my[me]

    def q_wait(hf):
        rows = pl.ds(hf * qh, qh)
        for k in range(1, 16):
            s_ = lax.rem(slot + k, 16)
            rcopy(q_in.at[s_, rows, :], q_in.at[s_, rows, :], c_s.at[hf, k - 1], c_r.at[hf, s_],
                  r, z, m).wait_recv()
        for s_ in range(16):
            qf[s_ * bl + hf * qh:s_ * bl + (hf + 1) * qh, :] = (
                q_in[s_, hf * qh:(hf + 1) * qh, :].astype(F32))

    w_pass_z(1)

    @pl.when(far)
    def _():
        w_y(1).start()

    w_pass_y(0)

    q_wait(0)

    lane = lax.broadcasted_iota(jnp.int32, (nh, t), 1)

    def query(b):
        return jnp.concatenate([qf[pl.ds(b, nh, stride=2 * bl), :],
                                qf[pl.ds(b + bl, nh, stride=2 * bl), :]], axis=1)

    def scores(b):
        return lax.dot_general(query(b).astype(BF), k_v[b], (((1,), (1,)), ((), ())),
                               preferred_element_type=F32) * scale

    def weights(b, s):
        s = jnp.where(lane < lens[start + b], s, -jnp.inf)
        sn = jnp.sum(query(b) * knf[pl.ds(b, 1), :], axis=1, keepdims=True) * scale
        top = jnp.maximum(jnp.max(s, axis=1, keepdims=True), sn)
        p = jnp.exp(s - top)
        pn = jnp.exp(sn - top)
        return p.astype(BF), pn, jnp.sum(p, axis=1, keepdims=True) + pn

    def values(b, bb, p, pn, l):
        acc = jnp.dot(p, v_v[b], preferred_element_type=F32)
        o = (acc + pn.astype(BF).astype(F32) * vnf[pl.ds(b, 1), :]) / l
        of[0, pl.ds(bb, nh, stride=nb), :] = o[:, :half]
        of[1, pl.ds(bb, nh, stride=nb), :] = o[:, half:]

    pos = z // 2
    og = pos * 2 + c

    def o_send(n, k):
        return rcopy(o_in.at[n, og], o_in.at[n, og], o_s.at[n, k], o_r.at[n, og],
                     r, z if k == 0 else z2, my if k == 0 else m)

    ng = (1 - pos) * 2 + c

    def o_pass(n):
        return rcopy(o_in.at[n, ng], o_in.at[n, ng], o_s.at[n, 2], o_r.at[n, ng], r, z, my)

    def o_rec(n, g):
        return rcopy(o_in.at[n, g], o_in.at[n, g], o_s.at[n, 0], o_r.at[n, g], r, z2, m)

    def o_mid(n):
        o_rec(n, ng).wait_recv()
        o_pass(n).start()

    def blk(n, zs, ms_):
        cols = pl.ds(pl.multiple_of((2 * (zs // 2) + ms_ % 2) * de, de), de)
        return y_v.at[:, zs % 2, pl.ds(2 * (ms_ // 2), 2), pl.ds(n * nb, nb), cols]

    others = (near, 2 - z // 2, 3 - 3 * (z // 2))

    def yz_send(n, k):
        return rcopy(blk(n, z, m), blk(n, z, m), yz_s.at[n, k], yz_r.at[n, z], r, others[k], m)

    inner = (z == 1) | (z == 2)
    ii = lax.rem((z + 1) // 2, 2)
    arrive = (near + ii * (others[1] - near), others[2] + ii * (near - others[2]),
              others[1] + ii * (others[2] - others[1]))

    def yz_pass(n):
        zs = others[1]
        return rcopy(blk(n, zs, m), blk(n, zs, m), yz_s.at[n, 3], yz_r.at[n, zs], r, near, m)

    def yz_rec(n, zs):
        return rcopy(blk(n, zs, m), blk(n, zs, m), yz_s.at[n, 0], yz_r.at[n, zs], r, near, m)

    def yy_send(n, zs):
        return rcopy(blk(n, zs, m), blk(n, zs, m), yy_s.at[n, zs], yy_r.at[n, zs], r, z, mx)

    def yy_rec(n, zs):
        return rcopy(blk(n, zs, mx), blk(n, zs, mx), yy_s.at[n, zs], yy_r.at[n, zs], r, z, mx)

    md = (1 - yy) * 2 + 1 - c

    def yd_send(n, zs, hop):
        ms_ = mx if hop else m
        return rcopy(blk(n, zs, ms_), blk(n, zs, ms_), yd_s.at[n, hop, zs], yd_r.at[n, hop, zs],
                     r, z, my)

    def yd_rec(n, zs, hop):
        ms_ = md if hop else my
        return rcopy(blk(n, zs, ms_), blk(n, zs, ms_), yd_s.at[n, hop, zs], yd_r.at[n, hop, zs],
                     r, z, my)

    def project(n):
        o_rec(n, pos * 2 + 1 - c).wait_recv()
        o_rec(n, (1 - pos) * 2 + 1 - c).wait_recv()
        ob = [o_in[n, g].astype(F32) for g in range(4)]
        lhs = jnp.concatenate(
            [jnp.concatenate([ob[g][h * nb:(h + 1) * nb] for g in range(4)], axis=0).astype(BF)
             for h in range(nh)], axis=1)
        acc = jnp.dot(lhs, wo_v[...].reshape(nh * dh, de), preferred_element_type=F32)
        cols = pl.ds(pl.multiple_of((2 * (z // 2) + c) * de, de), de)
        for g in range(4):
            mm = 2 * yy + g % 2
            row = ((z % 2 + 2 * (g // 2)) * 4 + mm) * bl
            xr = x_v[pl.ds(pl.multiple_of(row, bl), bl), cols].astype(F32)
            yb = xr[n * nb:(n + 1) * nb] + acc[g * nb:(g + 1) * nb]
            y_v[g // 2, z % 2, mm, n * nb:(n + 1) * nb, cols] = yb.astype(BF)
        @pl.when(~inner)
        def _():
            yz_send(n, 2).start()

        yz_send(n, 1).start()
        yz_send(n, 0).start()
        yy_send(n, z).start()
        yd_send(n, z, 0).start()

    def spread(n, zs):
        yy_send(n, zs).start()
        yd_send(n, zs, 0).start()

    def drain_z(n):
        for k, zs in enumerate(arrive):
            yz_rec(n, zs).wait_recv()
            if k == 0:
                @pl.when(inner)
                def _():
                    yz_pass(n).start()
            spread(n, zs)

    def drain_y(n):
        for zs in (z,) + others:
            yy_rec(n, zs).wait_recv()
            yd_send(n, zs, 1).start()

    s, p = {}, {}
    for i in range(bl + 2 * LAG):
        if i < bl:
            if i == qh:
                q_wait(1)
            if i % CHUNK == 0:
                kcp[i // CHUNK].wait()
                vcp[i // CHUNK].wait()
            s[i] = scores(i)
        if LAG <= i < bl + LAG:
            p[i - LAG] = weights(i - LAG, s.pop(i - LAG))
        if i >= 2 * LAG:
            b = i - 2 * LAG
            values(b, b % nb, *p.pop(b))
            if (b + 1) % nb == 0:
                n = b // nb
                o_in[n, og] = jnp.concatenate([of[0], of[1]], axis=1).astype(BF)
                o_send(n, 1).start()
                o_send(n, 0).start()
                if n > 1:
                    o_mid(n - 2)
                if n == 0:
                    w_pass_y(1)

    w_wait()
    project(0)
    project(1)
    o_mid(2)
    project(2)
    o_mid(3)
    project(3)
    drain_z(0)
    drain_z(1)
    drain_z(2)
    drain_z(3)
    drain_y(0)
    drain_y(1)
    drain_y(2)
    drain_y(3)
    for n in range(NB):
        for hop in range(2):
            for zs in range(4):
                yd_rec(n, zs, hop).wait_recv()

    a_each(lambda d, own: None if own else d.wait_send())
    for k in range(1, 4):
        for j in range(2):
            x_fwd(lax.rem(z + k, 4), j).wait_send()
    for hf in range(2):
        for k in range(1, 16):
            q_copy(hf, k).wait_send()
    @pl.when(far)
    def _():
        w_d2d.wait_send()
        for j in range(2):
            for k in range(2):
                w_next(k, j).wait_send()
            for mm in range(4):
                w_twin(mm, j).wait_send()

    for i in range(2):
        w_y(i).wait_send()
        w_z(i).wait_send()
    for n in range(NB):
        for k in range(2):
            o_send(n, k).wait_send()
        o_pass(n).wait_send()
        yz_send(n, 0).wait_send()
        yz_send(n, 1).wait_send()

        @pl.when(~inner)
        def _():
            yz_send(n, 2).wait_send()

        @pl.when(inner)
        def _():
            yz_pass(n).wait_send()

        for zs in range(4):
            yy_send(n, zs).wait_send()
            yd_send(n, zs, 0).wait_send()
            yd_send(n, zs, 1).wait_send()


def _store(y_v, kn_v, vn_v, y_h, kn_h, vn_h, sem):
    copies = [pltpu.make_async_copy(y_v, y_h, sem.at[0]),
              pltpu.make_async_copy(kn_v, kn_h, sem.at[1]),
              pltpu.make_async_copy(vn_v, vn_h, sem.at[2])]
    for copy in copies:
        copy.start()
    for copy in copies:
        copy.wait()


def solution(mesh):
    ne = mesh.shape['emb']
    nm = mesh.shape['model']

    def local(x, Wq, Wk, Wv, Wo, Kc, Vc, lengths):
        b, d = x.shape
        t, dh = Kc.shape[1:]
        de = Wq.shape[0]
        bl = b // (ne * nm)
        nb = bl // NB
        nh = 8
        hbm = pl.BlockSpec(memory_space=pl.ANY)
        vmem = pl.BlockSpec(memory_space=pltpu.VMEM)
        dma = pltpu.SemaphoreType.DMA
        y, kn, vn = pl.pallas_call(
            _kernel,
            out_shape=(pltpu.VMEM((2, ne // 2, nm, bl, d), BF), pltpu.VMEM((b, dh), BF),
                       pltpu.VMEM((b, dh), BF)),
            in_specs=[hbm] * 7 + [pl.BlockSpec(memory_space=pltpu.SMEM)],
            out_specs=(vmem, vmem, vmem),
            scratch_shapes=[
                pltpu.VMEM((b, d), BF), pltpu.VMEM(Wq.shape, BF), pltpu.VMEM((ne, de, dh // 2), BF),
                pltpu.VMEM(Wk.shape, BF), pltpu.VMEM(Wv.shape, BF), pltpu.VMEM(Wo.shape, BF),
                pltpu.VMEM((nm,) + Wo.shape, BF),
                pltpu.VMEM((bl, t, dh), BF), pltpu.VMEM((bl, t, dh), BF),
                pltpu.VMEM((bl, dh), F32), pltpu.VMEM((bl, dh), F32),
                pltpu.VMEM((b, dh // 2), F32),
                pltpu.VMEM((16, bl, dh // 2), BF), pltpu.VMEM((16, bl, dh // 2), BF),
                pltpu.VMEM((16 * bl, dh // 2), F32),
                pltpu.VMEM((2, nh * nb, dh // 2), F32),
                pltpu.VMEM((NB, 4, nh * nb, dh), BF),
                dma((6,)), dma((bl // CHUNK,)), dma((bl // CHUNK,)),
                dma((4, 2)), dma((4, 2)), dma((4, 2)), dma((4, 2)), dma((2, 15)), dma((2, 16)),
                dma((1,)), dma((1,)), dma((2,)), dma((2,)), dma((2, 2)), dma((4, 2)),
                dma((4, 2)), dma((4, 2)),
                dma((NB, 3)), dma((NB, 4)), dma((NB, 4)), dma((NB, 4)),
                dma((NB, 4)), dma((NB, 4)), dma((NB, 2, 4)), dma((NB, 2, 4)),
            ],
            compiler_params=pltpu.CompilerParams(
                collective_id=0, has_side_effects=True, vmem_limit_bytes=VMEM_LIMIT),
        )(x, Wq, Wk, Wv, Wo, Kc, Vc, lengths)
        y, kn, vn = (pltpu.with_memory_space_constraint(a, pltpu.VMEM) for a in (y.reshape(b, d), kn, vn))
        return pl.pallas_call(
            _store,
            out_shape=(jax.ShapeDtypeStruct((b, d), BF), jax.ShapeDtypeStruct((b, dh), BF),
                       jax.ShapeDtypeStruct((b, dh), BF)),
            in_specs=[vmem] * 3,
            out_specs=(hbm, hbm, hbm),
            scratch_shapes=[dma((3,))],
        )(y, kn, vn)

    in_specs = (P('rep', None), P('emb', 'model'), P(), P(), P('model', 'emb'),
                P('rep', None, None), P('rep', None, None), P('rep'))
    out_specs = (P('rep', None), P('rep', None), P('rep', None))
    return jax.shard_map(local, mesh=mesh, in_specs=in_specs, out_specs=out_specs, check_vma=False)
```
